32 devices in a mesh: high: 4 (over x, core), low: 8 (over z, y).
Axes of the slice: x: 2, y: 2, z: 4, core: 2. Of those that a mesh axis runs over, the one named last changes fastest.
Arguments:
- wave_parts: float32 [2, 512, 128, 128], P(None, ('high', 'low')), may hold values from -6 to 6
- level_table: float32 [512, 128, 128], P(('high', 'low')), may hold values from -2 to 2
- diagonal_angles: float32 [2, 128], replicated, may hold values from 0.3 to 1.2
- turn_angles: float32 [2, 4], replicated, may hold values from 0.3 to 1.2
Outputs:
- state_after: float32 [2, 512, 128, 128], P(None, ('high', 'low'))
The draws below stay inside these ranges and needn't reach their ends.
All inputs are finite; a program needn't handle non-finite values.
Results may differ from the reference program's by a relative error of at most 0.0003.
Values sent between devices are 32-bit elements.
A program may use at most 64 MiB of HBM per device.

```python
import jax
import jax.numpy as jnp
from jax import lax

BLOCKS_DEV = 16
ROWS = 128
LANES = 128
BLOCKS = 512
LAYERS = 2
N_HIGH = 4
N_LOW = 8


def block_scale(key, shape, cuts, least, high):
    level = 1.0
    for axis_at, shards_of in cuts:
        heights = jax.random.uniform(jax.random.fold_in(jax.random.fold_in(key, 6), axis_at), (shards_of,), jnp.float32, least / len(cuts), high / len(cuts))
        level = level * jnp.repeat(jnp.exp(heights), shape[axis_at] // shards_of).reshape((-1,) + (1,) * (len(shape) - 1 - axis_at))
    return level


def scatter_about(own_key, shape, deviation, reach, shards=(), kind=jnp.bfloat16):
    level = block_scale(own_key, shape, shards, -0.22, 0.18) if shards else 1.0
    array = jax.random.normal(own_key, shape, jnp.float32) * deviation * level
    return jnp.minimum(jnp.maximum(array, -reach), reach).astype(kind)


def setup_inputs(seed: int = 0) -> dict:
    key_of = jax.random.split(jax.random.key(seed), 5)
    return {
        "wave_parts": scatter_about(key_of[0], (2, BLOCKS, ROWS, LANES), 1.0, 6.0, ((1, 32),), jnp.float32),
        "level_table": jnp.clip(jax.random.uniform(key_of[1], (BLOCKS, ROWS, LANES), jnp.float32, -2.0, 2.0) * block_scale(key_of[1], (BLOCKS, ROWS, LANES), ((0, 32),), -0.4, 0.0), -2.0, 2.0),
        "diagonal_angles": jnp.clip(jax.random.uniform(key_of[2], (LAYERS, LANES), jnp.float32, 0.3, 1.2), 0.3, 1.2),
        "turn_angles": jnp.clip(jax.random.uniform(key_of[3], (LAYERS, 4), jnp.float32, 0.3, 1.2), 0.3, 1.2),
    }


def count_bits(values, count):
    places = jnp.arange(count.bit_length() - 1, dtype=jnp.int32)
    return jnp.sum((values[..., None] >> places) & 1, axis=-1)


def mix_table(count, angle):
    rank = jnp.arange(count, dtype=jnp.int32)
    apart = count_bits(rank[:, None] ^ rank[None, :], count)
    bits = count.bit_length() - 1
    size = jnp.cos(angle) ** (bits - apart).astype(jnp.float32) * jnp.sin(angle) ** apart.astype(jnp.float32)
    real_sign = jnp.where(apart % 4 == 0, 1.0, jnp.where(apart % 4 == 2, -1.0, 0.0)).astype(jnp.float32)
    imag_sign = jnp.where(apart % 4 == 1, -1.0, jnp.where(apart % 4 == 3, 1.0, 0.0)).astype(jnp.float32)
    return size * real_sign, size * imag_sign


def turn_dim(values, dim, angle):
    real_part, imag_part = mix_table(values.shape[dim], angle)
    def times(table):
        moved = jnp.tensordot(values, table, axes=([dim], [0]), precision=lax.Precision.HIGHEST)
        return jnp.moveaxis(moved, -1, dim)
    by_real = times(real_part)
    by_imag = times(imag_part)
    return jnp.stack([by_real[0] - by_imag[1], by_real[1] + by_imag[0]])


def diagonal_step(values, levels, angle):
    turn = angle * levels
    return jnp.stack([values[0] * jnp.cos(turn) + values[1] * jnp.sin(turn), values[1] * jnp.cos(turn) - values[0] * jnp.sin(turn)])


def reference(wave_parts, level_table, diagonal_angles, turn_angles):
    values = wave_parts
    for layer in range(LAYERS):
        values = diagonal_step(values, level_table, diagonal_angles[layer])
        values = turn_dim(values, 3, turn_angles[layer, 0])
        values = turn_dim(values, 2, turn_angles[layer, 1])
        parts = values.reshape(2, N_HIGH, N_LOW, BLOCKS_DEV, ROWS, LANES)
        parts = turn_dim(parts, 1, turn_angles[layer, 2])
        parts = turn_dim(parts, 2, turn_angles[layer, 3])
        parts = turn_dim(parts, 3, turn_angles[layer, 2])
        values = parts.reshape(values.shape)
    return values
```

```python
import functools

import jax
import jax.numpy as jnp
import numpy as np
from jax import lax
from jax.experimental import pallas as pl
from jax.experimental.pallas import tpu as pltpu
from jax.sharding import PartitionSpec as P

MESH = pl.DeviceIdType.MESH
F32 = jnp.float32
BF16 = jnp.bfloat16


def fit(function, powers, reach=3.2):
    x = np.cos(np.pi * (np.arange(4000) + 0.5) / 4000) * reach
    scaled = np.stack([(x / reach) ** p for p in powers], 1)
    found = np.linalg.lstsq(scaled, function(x), rcond=None)[0]
    return [float(f / reach**p) for f, p in zip(found, powers)]


SIN = fit(np.sin, range(1, 16, 2))
COS = fit(np.cos, range(0, 17, 2))


def cos_sin(x):
    z = x * x
    sine = jnp.full_like(x, SIN[-1])
    for f in SIN[-2::-1]:
        sine = sine * z + f
    cosine = jnp.full_like(x, COS[-1])
    for f in COS[-2::-1]:
        cosine = cosine * z + f
    return cosine, sine * x


def bits_of(count):
    return count.bit_length() - 1


def pop(values, bits):
    total = values % 2
    for q in range(1, bits):
        total = total + (values // 2**q) % 2
    return total


def pop_array(values, bits):
    total = values & 1
    for q in range(1, bits):
        total = total + ((values >> q) & 1)
    return total


def mix_list(xs, turns):
    for q, (c, s) in enumerate(turns):
        step = 1 << q
        ys = list(xs)
        for i in range(len(xs)):
            if not i & step:
                u, v = xs[i], xs[i + step]
                ys[i] = c * u - s * v
                ys[i + step] = s * u + c * v
        xs = ys
    return xs


def rotation(count, c, s, transposed):
    i = lax.broadcasted_iota(jnp.int32, (count, count), 0)
    j = lax.broadcasted_iota(jnp.int32, (count, count), 1)
    if transposed:
        i, j = j, i
    c, s = c[:1, :count], s[:1, :count]
    table = jnp.ones((count, count), F32)
    for q in range(bits_of(count)):
        a, b = (i >> q) & 1, (j >> q) & 1
        table = table * jnp.where(a == b, c, jnp.where(a == 1, s, -s))
    return table


def split(x):
    hi = x.astype(BF16)
    return hi, (x - hi.astype(F32)).astype(BF16)


def kernel(nh, nl, parts, wave_hbm, level_hbm, diag_hbm, turn_hbm, out,
           diag, turn, wave, level, abuf, recv, lev, back, home, lane_t, row_t,
           in_sem, lev_send, lev_recv, to_send, to_recv, ret_send, ret_recv):
    n = nh * nl
    blocks, rows, lanes = level.shape
    cut = n // blocks
    rp = rows // cut
    rq = rp // parts
    h, l = lax.axis_index("high"), lax.axis_index("low")
    me = h * nl + l

    def others(body):
        def step(k, carry):
            dh = lax.rem(h + k // nl, nh)
            dl = lax.rem(l + k % nl, nl)
            body(dh * nl + dl, (dh, dl))
            return carry
        lax.fori_loop(1, n, step, 0)

    level_in = pltpu.make_async_copy(level_hbm, level, in_sem.at[0])
    wave_in = pltpu.make_async_copy(wave_hbm, wave, in_sem.at[1])
    diag_in = pltpu.make_async_copy(diag_hbm, diag, in_sem.at[2])
    turn_in = pltpu.make_async_copy(turn_hbm, turn, in_sem.at[3])
    turn_in.start()
    diag_in.start()
    level_in.start()
    wave_in.start()

    barrier = pltpu.get_barrier_semaphore()
    others(lambda d, at: pl.semaphore_signal(barrier, inc=1, device_id=at, device_id_type=MESH))
    pl.semaphore_wait(barrier, n - 1)

    def own_rows(d):
        return pl.ds(pl.multiple_of((d % cut) * rp, 8), rp)

    def level_copy(d, at):
        return pltpu.make_async_remote_copy(
            src_ref=level_hbm.at[d // cut, own_rows(d)], dst_ref=lev.at[me],
            send_sem=lev_send.at[d], recv_sem=lev_recv.at[me],
            device_id=at, device_id_type=MESH)

    def to_copy(q):
        return lambda d, at: pltpu.make_async_remote_copy(
            src_ref=abuf.at[d, q], dst_ref=recv.at[me, q], send_sem=to_send.at[q, d],
            recv_sem=to_recv.at[q, me], device_id=at, device_id_type=MESH)

    def ret_copy(part, q):
        part_rows = pl.ds(q * rq, rq)
        return lambda d, at: pltpu.make_async_remote_copy(
            src_ref=back.at[d, part, part_rows], dst_ref=home.at[me, part, part_rows],
            send_sem=ret_send.at[part, q, d], recv_sem=ret_recv.at[part, q, me],
            device_id=at, device_id_type=MESH)

    def start_all(copy):
        others(lambda d, at: copy(d, at).start())

    def wait_all(block_of, sem):
        others(lambda d, at: pltpu.make_async_copy(block_of(d), block_of(d), sem.at[d]).wait())

    start_all(level_copy)

    turn_in.wait()
    diag_in.wait()

    turns = []
    for layer in range(2):
        turns.append([cos_sin(jnp.full((8, lanes), turn[layer, g], F32)) for g in range(4)])
        c, s = turns[layer][0]
        hi, lo = split(rotation(lanes, c, s, True))
        lane_t[layer] = jnp.concatenate(
            [jnp.concatenate([hi, lo], 1), jnp.concatenate([hi, jnp.zeros_like(hi)], 1)], 0)
        c, s = turns[layer][1]
        hi, lo = split(rotation(rows, c, s, False))
        row_t[layer] = jnp.concatenate(
            [jnp.concatenate([hi, hi], 1), jnp.concatenate([lo, jnp.zeros_like(hi)], 1)], 0)

    ones = pop_array(lax.broadcasted_iota(jnp.int32, (rows, lanes), 0), bits_of(rows)) + pop_array(
        lax.broadcasted_iota(jnp.int32, (rows, lanes), 1), bits_of(lanes))
    ones_dev = pop(me, bits_of(n))

    def mix_lanes(x, layer):
        hi, lo = split(x)
        z = jnp.dot(jnp.concatenate([hi, lo], 1), lane_t[layer], preferred_element_type=F32)
        return z[:, :lanes] + z[:, lanes:]

    def mix_rows(x, y, layer):
        hi, lo = split(jnp.concatenate([x, y], 1))
        z = jnp.dot(row_t[layer], jnp.concatenate([hi, lo], 0), preferred_element_type=F32)
        z = z[:rows] + z[rows:]
        return z[:, :lanes], z[:, lanes:]

    def mix_blocks(buf, middle_at, start, count, layer):
        pair = [turns[layer][2]] * bits_of(blocks)
        per = count // 8

        def body(t, carry):
            p, at = t // per, pl.ds(pl.multiple_of(start + (t % per) * 8, 8), 8)
            xs = mix_list([buf[b * cut + p, middle_at, at] for b in range(blocks)], pair)
            for b in range(blocks):
                buf[b * cut + p, middle_at, at] = xs[b]
            return carry
        lax.fori_loop(0, cut * per, body, 0)

    def quarter(b):
        k = (ones + (ones_dev + pop(b, bits_of(blocks)))) & 3
        return (k & 1) == 1, jnp.where(k >= 2, -1.0, 1.0)

    level_in.wait()
    wave_in.wait()
    lev[me] = level[me // cut, own_rows(me)]

    def first(b, carry):
        c, s = cos_sin(level[b] * diag[pl.ds(0, 1), :])
        odd, sign = quarter(b)
        cc = jnp.where(odd, s, c) * sign
        ss = jnp.where(odd, -c, s) * sign
        re, im = wave[0, b], wave[1, b]
        z = mix_lanes(jnp.concatenate([re * cc + im * ss, im * cc - re * ss], 0), 0)
        re, im = mix_rows(z[:rows], z[rows:], 0)
        for p in range(cut):
            for q in range(parts):
                at = p * rp + q * rq
                abuf[b * cut + p, q, :rq] = re[at:at + rq]
                abuf[b * cut + p, q, rq:] = im[at:at + rq]
        return carry
    lax.fori_loop(0, blocks, first, 0)
    for q in range(parts):
        mix_blocks(abuf, q, 0, 2 * rq, 0)
        start_all(to_copy(q))
        recv[me, q] = abuf[me, q]

    def dev_turns(layer):
        return [turns[layer][3]] * bits_of(nl) + [turns[layer][2]] * bits_of(nh)

    def middle(q):
        def body(j, carry):
            at = pl.ds(pl.multiple_of(j * 8, 8), 8)
            at_im = pl.ds(pl.multiple_of(rq + j * 8, 8), 8)
            at_part = pl.ds(pl.multiple_of(q * rq + j * 8, 8), 8)
            xs = mix_list([recv[d, q, at] for d in range(n)], dev_turns(0))
            for d in range(n):
                recv[d, q, at] = xs[d]
            ys = mix_list([recv[d, q, at_im] for d in range(n)], dev_turns(0))
            angle = diag[pl.ds(1, 1), :]
            for d in range(n):
                c, s = cos_sin(lev[d, at_part] * angle)
                x, y = recv[d, q, at], ys[d]
                recv[d, q, at] = x * c + y * s
                ys[d] = y * c - x * s
            ys = mix_list(ys, dev_turns(1))
            for d in range(n):
                back[d, 1, at_part] = ys[d]
            xs = mix_list([recv[d, q, at] for d in range(n)], dev_turns(1))
            for d in range(n):
                back[d, 0, at_part] = xs[d]
            return carry
        lax.fori_loop(0, rq // 8, body, 0)

    def middle_lanes(part, q):
        group = min(n, 256 // rq)
        at = pl.ds(q * rq, rq)
        for i in range(n // group):
            ds = pl.ds(i * group, group)
            z = mix_lanes(back[ds, part, at].reshape(group * rq, lanes), 1)
            back[ds, part, at] = z.reshape(group, rq, lanes)

    wait_all(lambda d: lev.at[d], lev_recv)
    for q in range(parts):
        wait_all(lambda d: recv.at[d, q], to_recv.at[q])
        middle(q)
        middle_lanes(0, q)
        start_all(ret_copy(0, q))
        middle_lanes(1, q)
    for q in range(parts):
        start_all(ret_copy(1, q))
    home[me] = back[me]

    def gather(b, part):
        return jnp.concatenate([home[b * cut + p, part] for p in range(cut)], 0)


    for part in range(2):
        for q in range(parts):
            wait_all(lambda d: home.at[d, part, pl.ds(q * rq, rq)], ret_recv.at[part, q])
            mix_blocks(home, part, q * rq, rq, 1)

        def last(i, carry):
            b = 2 * i
            for at, x in zip((b, b + 1), mix_rows(gather(b, part), gather(b + 1, part), 1)):
                if part == 0:
                    wave[0, at] = x
                else:
                    odd, sign = quarter(at)
                    re = wave[0, at]
                    out[0, at] = jnp.where(odd, x, re) * sign
                    out[1, at] = jnp.where(odd, -re, x) * sign
            return carry
        lax.fori_loop(0, blocks // 2, last, 0, unroll=4)

    def drain(d, at):
        level_copy(d, at).wait_send()
        for q in range(parts):
            to_copy(q)(d, at).wait_send()
            for part in range(2):
                ret_copy(part, q)(d, at).wait_send()
    others(drain)


def put_out(done, out, sem):
    blocks = done.shape[1]
    copies = []
    for part in range(2):
        for q in range(2):
            at = pl.ds(q * (blocks // 2), blocks // 2)
            copies.append(pltpu.make_async_copy(done.at[part, at], out.at[part, at], sem.at[2 * part + q]))
    for copy in copies:
        copy.start()
    for copy in copies:
        copy.wait()


def solution(mesh):
    nh, nl = mesh.shape["high"], mesh.shape["low"]
    n = nh * nl

    def on_device(wave, level, diag, turn):
        blocks, rows, lanes = level.shape
        rp = rows // (n // blocks)
        parts = 2 if rp % 16 == 0 else 1
        hbm = pl.BlockSpec(memory_space=pltpu.HBM)
        dma = pltpu.SemaphoreType.DMA
        done = pl.pallas_call(
            functools.partial(kernel, nh, nl, parts),
            out_shape=pltpu.VMEM(wave.shape, F32),
            in_specs=[hbm] * 4,
            out_specs=pl.BlockSpec(memory_space=pltpu.VMEM),
            scratch_shapes=[
                pltpu.VMEM(diag.shape, F32),
                pltpu.SMEM(turn.shape, F32),
                pltpu.VMEM(wave.shape, F32),
                pltpu.VMEM(level.shape, F32),
                pltpu.VMEM((n, parts, 2 * rp // parts, lanes), F32),
                pltpu.VMEM((n, parts, 2 * rp // parts, lanes), F32),
                pltpu.VMEM((n, rp, lanes), F32),
                pltpu.VMEM((n, 2, rp, lanes), F32),
                pltpu.VMEM((n, 2, rp, lanes), F32),
                pltpu.VMEM((2, 2 * lanes, 2 * lanes), BF16),
                pltpu.VMEM((2, 2 * rows, 2 * rows), BF16),
                dma((4,)), dma((n,)), dma((n,)), dma((parts, n)), dma((parts, n)),
                dma((2, parts, n)), dma((2, parts, n)),
            ],
            compiler_params=pltpu.CompilerParams(
                collective_id=0, has_side_effects=True, vmem_limit_bytes=20 * 2**20),
        )(*[pltpu.with_memory_space_constraint(x, pltpu.HBM) for x in (wave, level, diag, turn)])
        return pl.pallas_call(
            put_out,
            out_shape=jax.ShapeDtypeStruct(wave.shape, F32),
            in_specs=[pl.BlockSpec(memory_space=pltpu.VMEM)],
            out_specs=hbm,
            scratch_shapes=[dma((4,))],
            compiler_params=pltpu.CompilerParams(vmem_limit_bytes=2**20),
        )(done)

    in_specs = (P(None, ("high", "low"), None, None), P(("high", "low"), None, None), P(), P())
    return jax.shard_map(
        on_device, mesh=mesh, in_specs=in_specs,
        out_specs=P(None, ("high", "low"), None, None), check_vma=False)
```

```python
import functools

import jax
import jax.numpy as jnp
import numpy as np
from jax import lax
from jax.experimental import pallas as pl
from jax.experimental.pallas import tpu as pltpu
from jax.sharding import PartitionSpec as P

MESH = pl.DeviceIdType.MESH
F32 = jnp.float32
BF16 = jnp.bfloat16


def fit(function, powers, reach=3.2):
    x = np.cos(np.pi * (np.arange(4000) + 0.5) / 4000) * reach
    scaled = np.stack([(x / reach) ** p for p in powers], 1)
    found = np.linalg.lstsq(scaled, function(x), rcond=None)[0]
    return [float(f / reach**p) for f, p in zip(found, powers)]


SIN = fit(np.sin, range(1, 16, 2))
COS = fit(np.cos, range(0, 17, 2))


def cos_sin(x):
    z = x * x
    sine = jnp.full_like(x, SIN[-1])
    for f in SIN[-2::-1]:
        sine = sine * z + f
    cosine = jnp.full_like(x, COS[-1])
    for f in COS[-2::-1]:
        cosine = cosine * z + f
    return cosine, sine * x


def bits_of(count):
    return count.bit_length() - 1


def pop(values, bits):
    total = values % 2
    for q in range(1, bits):
        total = total + (values // 2**q) % 2
    return total


def pop_array(values, bits):
    total = values & 1
    for q in range(1, bits):
        total = total + ((values >> q) & 1)
    return total


def mix_list(xs, turns):
    for q, (c, s) in enumerate(turns):
        step = 1 << q
        ys = list(xs)
        for i in range(len(xs)):
            if not i & step:
                u, v = xs[i], xs[i + step]
                ys[i] = c * u - s * v
                ys[i + step] = s * u + c * v
        xs = ys
    return xs


def rotation(count, c, s, transposed):
    i = lax.broadcasted_iota(jnp.int32, (count, count), 0)
    j = lax.broadcasted_iota(jnp.int32, (count, count), 1)
    if transposed:
        i, j = j, i
    c, s = c[:1, :count], s[:1, :count]
    table = jnp.ones((count, count), F32)
    for q in range(bits_of(count)):
        a, b = (i >> q) & 1, (j >> q) & 1
        table = table * jnp.where(a == b, c, jnp.where(a == 1, s, -s))
    return table


def split(x):
    hi = x.astype(BF16)
    return hi, (x - hi.astype(F32)).astype(BF16)


def kernel(nh, nl, parts, wave_hbm, level_hbm, diag_hbm, turn_hbm, out,
           diag, turn, wave, level, abuf, recv, lev, back, home, lane_t, row_t,
           in_sem, ready, lev_send, lev_recv, to_send, to_recv, ret_send, ret_recv):
    n = nh * nl
    blocks, rows, lanes = level.shape
    cut = n // blocks
    rp = rows // cut
    rq = rp // parts
    h, l = lax.axis_index("high"), lax.axis_index("low")
    me = h * nl + l

    quad = nl // 4
    plane = nh * quad

    def others(body, start=0):
        def step(k, carry):
            dh = h ^ (nh - 1 - k % nh)
            dl = l ^ (nl - 1 - k // nh)
            body(dh * nl + dl, (dh, dl))
            return carry
        lax.fori_loop(start, n - 1, step, 0)

    def line(body, first):
        for j in range(first, 4):
            dl = l ^ (j * quad)
            body(h * nl + dl, (h, dl))

    def near(body):
        others(body, n - plane)

    def off_line(body):
        def step(k, carry):
            dh = h ^ (nh - 1 - k % (nh - 1))
            dl = l ^ (nl - 1 - k // (nh - 1))
            body(dh * nl + dl, (dh, dl))
            return carry
        lax.fori_loop(0, nl * (nh - 1), step, 0)

        def column(k, carry):
            dl = l ^ (k + k // (quad - 1) + 1) if quad > 1 else l
            body(h * nl + dl, (h, dl))
            return carry
        lax.fori_loop(0, 4 * (quad - 1), column, 0)

    level_in = pltpu.make_async_copy(level_hbm, level, in_sem.at[0])
    wave_in = pltpu.make_async_copy(wave_hbm, wave, in_sem.at[1])
    diag_in = pltpu.make_async_copy(diag_hbm, diag, in_sem.at[2])
    turn_in = pltpu.make_async_copy(turn_hbm, turn, in_sem.at[3])
    level_in.start()
    turn_in.start()
    diag_in.start()
    wave_in.start()

    barrier = pltpu.get_barrier_semaphore()

    def greet(sem):
        return lambda d, at: pl.semaphore_signal(sem, inc=1, device_id=at, device_id_type=MESH)

    line(greet(barrier), 1)
    near(greet(barrier))
    level_in.wait()
    pl.semaphore_wait(barrier, plane + 2)

    def own_rows(d):
        return pl.ds(pl.multiple_of((d % cut) * rp, 8), rp)

    def level_copy(d, at):
        return pltpu.make_async_remote_copy(
            src_ref=level.at[d // cut, own_rows(d)], dst_ref=lev.at[me],
            send_sem=lev_send, recv_sem=lev_recv,
            device_id=at, device_id_type=MESH)

    def to_copy(q):
        return lambda d, at: pltpu.make_async_remote_copy(
            src_ref=abuf.at[d, q], dst_ref=recv.at[me, q], send_sem=to_send.at[q],
            recv_sem=to_recv.at[q], device_id=at, device_id_type=MESH)

    def ret_copy(part, q):
        part_rows = pl.ds(q * rq, rq)
        return lambda d, at: pltpu.make_async_remote_copy(
            src_ref=back.at[d, part, part_rows], dst_ref=home.at[me, part, part_rows],
            send_sem=ret_send.at[part, q], recv_sem=ret_recv.at[part, q],
            device_id=at, device_id_type=MESH)

    def start_all(copy):
        others(lambda d, at: copy(d, at).start())

    def wait_all(blocks_of, sem):
        most = blocks_of(pl.ds(0, n - 1))
        pltpu.make_async_copy(most, most, sem).wait()

    line(lambda d, at: level_copy(d, at).start(), 2)
    near(greet(ready))
    pl.semaphore_wait(ready, plane - 1)
    dl = l ^ quad
    level_copy(h * nl + dl, (h, dl)).start()
    off_line(lambda d, at: level_copy(d, at).start())

    turn_in.wait()
    diag_in.wait()

    turns = []
    for layer in range(2):
        turns.append([cos_sin(jnp.full((8, lanes), turn[layer, g], F32)) for g in range(4)])
        c, s = turns[layer][0]
        hi, lo = split(rotation(lanes, c, s, True))
        lane_t[layer] = jnp.concatenate(
            [jnp.concatenate([hi, lo], 1), jnp.concatenate([hi, jnp.zeros_like(hi)], 1)], 0)
        c, s = turns[layer][1]
        hi, lo = split(rotation(rows, c, s, False))
        row_t[layer] = jnp.concatenate(
            [jnp.concatenate([hi, hi], 1), jnp.concatenate([lo, jnp.zeros_like(hi)], 1)], 0)

    ones = pop_array(lax.broadcasted_iota(jnp.int32, (rows, lanes), 0), bits_of(rows)) + pop_array(
        lax.broadcasted_iota(jnp.int32, (rows, lanes), 1), bits_of(lanes))
    ones_dev = pop(me, bits_of(n))

    def mix_lanes(x, layer):
        hi, lo = split(x)
        z = jnp.dot(jnp.concatenate([hi, lo], 1), lane_t[layer], preferred_element_type=F32)
        return z[:, :lanes] + z[:, lanes:]

    def mix_rows(x, y, layer):
        hi, lo = split(jnp.concatenate([x, y], 1))
        z = jnp.dot(row_t[layer], jnp.concatenate([hi, lo], 0), preferred_element_type=F32)
        z = z[:rows] + z[rows:]
        return z[:, :lanes], z[:, lanes:]

    def mix_blocks(buf, middle_at, start, count, layer):
        pair = [turns[layer][2]] * bits_of(blocks)
        per = count // 8

        def body(t, carry):
            p, at = t // per, pl.ds(pl.multiple_of(start + (t % per) * 8, 8), 8)
            xs = mix_list([buf[b * cut + p, middle_at, at] for b in range(blocks)], pair)
            for b in range(blocks):
                buf[b * cut + p, middle_at, at] = xs[b]
            return carry
        lax.fori_loop(0, cut * per, body, 0)

    def quarter(b):
        k = (ones + (ones_dev + pop(b, bits_of(blocks)))) & 3
        return (k & 1) == 1, jnp.where(k >= 2, -1.0, 1.0)

    wave_in.wait()
    lev[me] = level[me // cut, own_rows(me)]

    def first(b, carry):
        c, s = cos_sin(level[b] * diag[pl.ds(0, 1), :])
        odd, sign = quarter(b)
        cc = jnp.where(odd, s, c) * sign
        ss = jnp.where(odd, -c, s) * sign
        re, im = wave[0, b], wave[1, b]
        z = mix_lanes(jnp.concatenate([re * cc + im * ss, im * cc - re * ss], 0), 0)
        re, im = mix_rows(z[:rows], z[rows:], 0)
        for p in range(cut):
            for q in range(parts):
                at = p * rp + q * rq
                abuf[b * cut + p, q, :rq] = re[at:at + rq]
                abuf[b * cut + p, q, rq:] = im[at:at + rq]
        return carry
    lax.fori_loop(0, blocks, first, 0)
    for q in range(parts):
        mix_blocks(abuf, q, 0, 2 * rq, 0)
        start_all(to_copy(q))
        recv[me, q] = abuf[me, q]

    def dev_turns(layer):
        return [turns[layer][3]] * bits_of(nl) + [turns[layer][2]] * bits_of(nh)

    def middle(q):
        def body(j, carry):
            at = pl.ds(pl.multiple_of(j * 8, 8), 8)
            at_im = pl.ds(pl.multiple_of(rq + j * 8, 8), 8)
            at_part = pl.ds(pl.multiple_of(q * rq + j * 8, 8), 8)
            xs = mix_list([recv[d, q, at] for d in range(n)], dev_turns(0))
            for d in range(n):
                recv[d, q, at] = xs[d]
            ys = mix_list([recv[d, q, at_im] for d in range(n)], dev_turns(0))
            angle = diag[pl.ds(1, 1), :]
            for d in range(n):
                c, s = cos_sin(lev[d, at_part] * angle)
                x, y = recv[d, q, at], ys[d]
                recv[d, q, at] = x * c + y * s
                ys[d] = y * c - x * s
            ys = mix_list(ys, dev_turns(1))
            for d in range(n):
                back[d, 1, at_part] = ys[d]
            xs = mix_list([recv[d, q, at] for d in range(n)], dev_turns(1))
            for d in range(n):
                back[d, 0, at_part] = xs[d]
            return carry
        lax.fori_loop(0, rq // 8, body, 0)

    def middle_lanes(part, q):
        group = min(n, 256 // rq)
        at = pl.ds(q * rq, rq)
        for i in range(n // group):
            ds = pl.ds(i * group, group)
            z = mix_lanes(back[ds, part, at].reshape(group * rq, lanes), 1)
            back[ds, part, at] = z.reshape(group, rq, lanes)

    wait_all(lambda d: lev.at[d], lev_recv)
    for q in range(parts):
        wait_all(lambda d: recv.at[d, q], to_recv.at[q])
        middle(q)
        middle_lanes(0, q)
        start_all(ret_copy(0, q))
        middle_lanes(1, q)
    for q in range(parts):
        start_all(ret_copy(1, q))
    home[me] = back[me]

    wait_all(lambda d: lev.at[d], lev_send)
    for q in range(parts):
        wait_all(lambda d: abuf.at[d, q], to_send.at[q])

    def gather(b, part):
        return jnp.concatenate([home[b * cut + p, part] for p in range(cut)], 0)


    for part in range(2):
        for q in range(parts):
            wait_all(lambda d: home.at[d, part, pl.ds(q * rq, rq)], ret_recv.at[part, q])
            mix_blocks(home, part, q * rq, rq, 1)

        def last(i, carry):
            b = 2 * i
            for at, x in zip((b, b + 1), mix_rows(gather(b, part), gather(b + 1, part), 1)):
                if part == 0:
                    wave[0, at] = x
                else:
                    odd, sign = quarter(at)
                    re = wave[0, at]
                    out[0, at] = jnp.where(odd, x, re) * sign
                    out[1, at] = jnp.where(odd, -re, x) * sign
            return carry
        lax.fori_loop(0, blocks // 2, last, 0, unroll=4)
    for q in range(parts):
        for part in range(2):
            wait_all(lambda d: back.at[d, part, pl.ds(q * rq, rq)], ret_send.at[part, q])


def put_out(done, out, sem):
    blocks = done.shape[1]
    copies = []
    for part in range(2):
        for q in range(2):
            at = pl.ds(q * (blocks // 2), blocks // 2)
            copies.append(pltpu.make_async_copy(done.at[part, at], out.at[part, at], sem.at[2 * part + q]))
    for copy in copies:
        copy.start()
    for copy in copies:
        copy.wait()


def solution(mesh):
    nh, nl = mesh.shape["high"], mesh.shape["low"]
    n = nh * nl

    def on_device(wave, level, diag, turn):
        blocks, rows, lanes = level.shape
        rp = rows // (n // blocks)
        parts = 2 if rp % 16 == 0 else 1
        hbm = pl.BlockSpec(memory_space=pltpu.HBM)
        dma = pltpu.SemaphoreType.DMA
        done = pl.pallas_call(
            functools.partial(kernel, nh, nl, parts),
            out_shape=pltpu.VMEM(wave.shape, F32),
            in_specs=[hbm] * 4,
            out_specs=pl.BlockSpec(memory_space=pltpu.VMEM),
            scratch_shapes=[
                pltpu.VMEM(diag.shape, F32),
                pltpu.SMEM(turn.shape, F32),
                pltpu.VMEM(wave.shape, F32),
                pltpu.VMEM(level.shape, F32),
                pltpu.VMEM((n, parts, 2 * rp // parts, lanes), F32),
                pltpu.VMEM((n, parts, 2 * rp // parts, lanes), F32),
                pltpu.VMEM((n, rp, lanes), F32),
                pltpu.VMEM((n, 2, rp, lanes), F32),
                pltpu.VMEM((n, 2, rp, lanes), F32),
                pltpu.VMEM((2, 2 * lanes, 2 * lanes), BF16),
                pltpu.VMEM((2, 2 * rows, 2 * rows), BF16),
                dma((4,)), pltpu.SemaphoreType.REGULAR, dma, dma, dma((parts,)), dma((parts,)),
                dma((2, parts)), dma((2, parts)),
            ],
            compiler_params=pltpu.CompilerParams(
                collective_id=0, has_side_effects=True, vmem_limit_bytes=20 * 2**20),
        )(*[pltpu.with_memory_space_constraint(x, pltpu.HBM) for x in (wave, level, diag, turn)])
        return pl.pallas_call(
            put_out,
            out_shape=jax.ShapeDtypeStruct(wave.shape, F32),
            in_specs=[pl.BlockSpec(memory_space=pltpu.VMEM)],
            out_specs=hbm,
            scratch_shapes=[dma((4,))],
            compiler_params=pltpu.CompilerParams(vmem_limit_bytes=2**20),
        )(done)

    in_specs = (P(None, ("high", "low"), None, None), P(("high", "low"), None, None), P(), P())
    return jax.shard_map(
        on_device, mesh=mesh, in_specs=in_specs,
        out_specs=P(None, ("high", "low"), None, None), check_vma=False)
```

```python
import functools

import jax
import jax.numpy as jnp
import numpy as np
from jax import lax
from jax.experimental import pallas as pl
from jax.experimental.pallas import tpu as pltpu
from jax.sharding import PartitionSpec as P

MESH = pl.DeviceIdType.MESH
F32 = jnp.float32
BF16 = jnp.bfloat16


def fit(function, powers, reach=3.2):
    x = np.cos(np.pi * (np.arange(4000) + 0.5) / 4000) * reach
    scaled = np.stack([(x / reach) ** p for p in powers], 1)
    found = np.linalg.lstsq(scaled, function(x), rcond=None)[0]
    return [float(f / reach**p) for f, p in zip(found, powers)]


SIN = fit(np.sin, range(1, 16, 2))
COS = fit(np.cos, range(0, 17, 2))


def cos_sin(x):
    z = x * x
    sine = jnp.full_like(x, SIN[-1])
    for f in SIN[-2::-1]:
        sine = sine * z + f
    cosine = jnp.full_like(x, COS[-1])
    for f in COS[-2::-1]:
        cosine = cosine * z + f
    return cosine, sine * x


def bits_of(count):
    return count.bit_length() - 1


def pop(values, bits):
    total = values % 2
    for q in range(1, bits):
        total = total + (values // 2**q) % 2
    return total


def pop_array(values, bits):
    total = values & 1
    for q in range(1, bits):
        total = total + ((values >> q) & 1)
    return total


def mix_list(xs, turns):
    for q, (c, s) in enumerate(turns):
        step = 1 << q
        ys = list(xs)
        for i in range(len(xs)):
            if not i & step:
                u, v = xs[i], xs[i + step]
                ys[i] = c * u - s * v
                ys[i + step] = s * u + c * v
        xs = ys
    return xs


def rotation(count, c, s, transposed, mixed):
    i = lax.broadcasted_iota(jnp.int32, (count, count), 0)
    j = lax.broadcasted_iota(jnp.int32, (count, count), 1)
    if transposed:
        i, j = j, i
    c, s = c[:1, :count], s[:1, :count]
    table = jnp.where((i >> mixed) == (j >> mixed), 1.0, 0.0)
    for q in range(mixed):
        a, b = (i >> q) & 1, (j >> q) & 1
        table = table * jnp.where(a == b, c, jnp.where(a == 1, s, -s))
    return table


def split(x):
    hi = x.astype(BF16)
    return hi, (x - hi.astype(F32)).astype(BF16)


def kernel(nh, nl, parts, wave_hbm, level_hbm, diag_hbm, turn_hbm, out,
           diag, turn, wave, level, abuf, recv, lev, back, home, lane_t, row_t,
           in_sem, ready, lev_send, lev_recv, to_send, to_recv, ret_send, ret_recv):
    n = nh * nl
    blocks, rows, lanes = level.shape
    cut = n // blocks
    rp = rows // cut
    rq = rp // parts
    h, l = lax.axis_index("high"), lax.axis_index("low")
    me = h * nl + l

    quad = nl // 4
    plane = nh * quad

    zi, yi = l // quad, l % quad

    def call(body, dh, dl):
        body(dh * nl + dl, (dh, dl))

    def far_line(j):
        return jnp.where(zi < 2, 3 - j, j) * quad

    def far(body):
        def step(k, carry):
            t = k // nh
            call(body, h ^ (nh - 1 - k % nh), far_line(t // quad) + (yi ^ (quad - 1 - t % quad)))
            return carry
        lax.fori_loop(0, n // 2, step, 0)

    def near(body, count=n // 2 - 1):
        def step(k, carry):
            call(body, h ^ (nh - 1 - k % nh), l ^ (nl // 2 - 1 - k // nh))
            return carry
        lax.fori_loop(n // 2 - 1 - count, n // 2 - 1, step, 0)

    def others(body):
        near(body)
        far(body)

    def off_line(body):
        def step(k, carry):
            t = k // (nh - 1)
            call(body, h ^ (nh - 1 - k % (nh - 1)), far_line(t // quad) + (yi ^ (quad - 1 - t % quad)))
            return carry
        lax.fori_loop(0, (nh - 1) * 2 * quad, step, 0)

        def column(k, carry):
            t = k // (quad - 1)
            call(body, h, far_line(t) + (yi ^ (quad - 1 - k % (quad - 1))))
            return carry
        if quad > 1:
            lax.fori_loop(0, 2 * (quad - 1), column, 0)

    level_in = pltpu.make_async_copy(level_hbm, level, in_sem.at[0])
    wave_in = pltpu.make_async_copy(wave_hbm, wave, in_sem.at[1])
    diag_in = pltpu.make_async_copy(diag_hbm, diag, in_sem.at[2])
    turn_in = pltpu.make_async_copy(turn_hbm, turn, in_sem.at[3])
    level_in.start()
    turn_in.start()
    diag_in.start()
    wave_in.start()

    barrier = pltpu.get_barrier_semaphore()

    def greet(sem):
        return lambda d, at: pl.semaphore_signal(sem, inc=1, device_id=at, device_id_type=MESH)

    for j in range(1, 4):
        call(greet(barrier), h, l ^ (j * quad))
    near(greet(barrier), plane - 1)
    level_in.wait()
    pl.semaphore_wait(barrier, plane + 2)

    def own_rows(d):
        return pl.ds(pl.multiple_of((d % cut) * rp, 8), rp)

    def level_copy(d, at):
        return pltpu.make_async_remote_copy(
            src_ref=level.at[d // cut, own_rows(d)], dst_ref=lev.at[me],
            send_sem=lev_send, recv_sem=lev_recv,
            device_id=at, device_id_type=MESH)

    def to_copy(q):
        return lambda d, at: pltpu.make_async_remote_copy(
            src_ref=abuf.at[d, q], dst_ref=recv.at[me, q], send_sem=to_send.at[q],
            recv_sem=to_recv.at[q], device_id=at, device_id_type=MESH)

    pieces = [(q, 0, 2) for q in range(parts - 1)] + [(parts - 1, 0, 1), (parts - 1, 1, 1)]

    def piece_of(buf, d, i):
        q, part, count = pieces[i]
        return buf.at[d, q, pl.ds(part, count)]

    def ret_copy(i):
        return lambda d, at: pltpu.make_async_remote_copy(
            src_ref=piece_of(back, d, i), dst_ref=piece_of(home, me, i),
            send_sem=ret_send.at[i], recv_sem=ret_recv.at[i],
            device_id=at, device_id_type=MESH)

    def wait_all(blocks_of, sem):
        most = blocks_of(pl.ds(0, n - 1))
        pltpu.make_async_copy(most, most, sem).wait()

    def start(copy):
        return lambda d, at: copy(d, at).start()

    for j in range(2):
        call(start(level_copy), h, far_line(j) + yi)
    near(greet(ready), plane - 1)
    pl.semaphore_wait(ready, plane - 1)
    off_line(start(level_copy))
    near(start(level_copy))

    turn_in.wait()
    diag_in.wait()

    turns = []
    for layer in range(2):
        turns.append([cos_sin(jnp.full((8, lanes), turn[layer, g], F32)) for g in range(4)])
        c, s = turns[layer][0]
        hi, lo = split(rotation(lanes, c, s, True, bits_of(lanes)))
        lane_t[layer] = jnp.concatenate(
            [jnp.concatenate([hi, lo], 1), jnp.concatenate([hi, jnp.zeros_like(hi)], 1)], 0)
        c, s = turns[layer][1]
        hi, lo = split(rotation(rows, c, s, False, bits_of(rows if layer == 0 else rq)))
        row_t[layer] = jnp.concatenate(
            [jnp.concatenate([hi, hi], 1), jnp.concatenate([lo, jnp.zeros_like(hi)], 1)], 0)

    ones = pop_array(lax.broadcasted_iota(jnp.int32, (rows, lanes), 0), bits_of(rows)) + pop_array(
        lax.broadcasted_iota(jnp.int32, (rows, lanes), 1), bits_of(lanes))
    ones_dev = pop(me, bits_of(n))

    def mix_lanes(x, layer):
        hi, lo = split(x)
        z = jnp.dot(jnp.concatenate([hi, lo], 1), lane_t[layer], preferred_element_type=F32)
        return z[:, :lanes] + z[:, lanes:]

    def mix_rows(x, y, layer):
        hi, lo = split(jnp.concatenate([x, y], 1))
        z = jnp.dot(row_t[layer], jnp.concatenate([hi, lo], 0), preferred_element_type=F32)
        z = z[:rows] + z[rows:]
        return z[:, :lanes], z[:, lanes:]

    def mix_blocks(buf, middle_at, start, count, layer):
        pair = [turns[layer][2]] * bits_of(blocks)
        per = count // 8

        def body(t, carry):
            p, at = t // per, pl.ds(pl.multiple_of(start + (t % per) * 8, 8), 8)
            xs = mix_list([buf[b * cut + p, middle_at, at] for b in range(blocks)], pair)
            for b in range(blocks):
                buf[b * cut + p, middle_at, at] = xs[b]
            return carry
        lax.fori_loop(0, cut * per, body, 0)

    def quarter(count):
        k = (ones + count) & 3
        return (k & 1) == 1, jnp.where(k >= 2, -1.0, 1.0)

    wave_in.wait()
    lev[me] = level[me // cut, own_rows(me)]

    def first(b, carry):
        c, s = cos_sin(level[b] * diag[pl.ds(0, 1), :])
        odd, sign = quarter(ones_dev + pop(b, bits_of(blocks)))
        cc = jnp.where(odd, s, c) * sign
        ss = jnp.where(odd, -c, s) * sign
        re, im = wave[0, b], wave[1, b]
        z = mix_lanes(jnp.concatenate([re * cc + im * ss, im * cc - re * ss], 0), 0)
        re, im = mix_rows(z[:rows], z[rows:], 0)
        for p in range(cut):
            for q in range(parts):
                at = p * rp + q * rq
                abuf[b * cut + p, q, :rq] = re[at:at + rq]
                abuf[b * cut + p, q, rq:] = im[at:at + rq]
        return carry
    lax.fori_loop(0, blocks, first, 0)
    for q in range(parts):
        mix_blocks(abuf, q, 0, 2 * rq, 0)
        others(start(to_copy(q)))
        recv[me, q] = abuf[me, q]

    def dev_turns(layer):
        return [turns[layer][3]] * bits_of(nl) + [turns[layer][2]] * bits_of(nh)

    def middle(q):
        def body(j, carry):
            at = pl.ds(pl.multiple_of(j * 8, 8), 8)
            at_im = pl.ds(pl.multiple_of(rq + j * 8, 8), 8)
            at_part = pl.ds(pl.multiple_of(q * rq + j * 8, 8), 8)
            xs = mix_list([recv[d, q, at] for d in range(n)], dev_turns(0))
            for d in range(n):
                recv[d, q, at] = xs[d]
            ys = mix_list([recv[d, q, at_im] for d in range(n)], dev_turns(0))
            angle = diag[pl.ds(1, 1), :]
            for d in range(n):
                c, s = cos_sin(lev[d, at_part] * angle)
                x, y = recv[d, q, at], ys[d]
                recv[d, q, at] = x * c + y * s
                ys[d] = y * c - x * s
            ys = mix_list(ys, dev_turns(1))
            for d in range(n):
                back[d, q, 1, at] = ys[d]
            xs = mix_list([recv[d, q, at] for d in range(n)], dev_turns(1))
            for d in range(n):
                back[d, q, 0, at] = xs[d]
            return carry
        lax.fori_loop(0, rq // 8, body, 0)

    group = rows // rq

    def finish(q):
        def body(i, carry):
            ds = pl.ds(i * group, group)
            z = [back[ds, q, part].reshape(rows, lanes) for part in range(2)]
            z = mix_lanes(jnp.concatenate(z, 0), 1)
            re, im = mix_rows(z[:rows], z[rows:], 1)
            odd, sign = quarter(pop(i, bits_of(n // group)))
            back[ds, q, 0] = (jnp.where(odd, im, re) * sign).reshape(group, rq, lanes)
            back[ds, q, 1] = (jnp.where(odd, -re, im) * sign).reshape(group, rq, lanes)
            return carry
        lax.fori_loop(0, n // group, body, 0, unroll=2)

    wait_all(lambda d: lev.at[d], lev_recv)
    for q in range(parts):
        wait_all(lambda d: recv.at[d, q], to_recv.at[q])
        middle(q)
        finish(q)
        for i, piece in enumerate(pieces):
            if piece[0] == q:
                others(start(ret_copy(i)))
    home[me] = back[me]

    wait_all(lambda d: lev.at[d], lev_send)
    for q in range(parts):
        wait_all(lambda d: abuf.at[d, q], to_send.at[q])

    own_turns = [turns[1][1]] * bits_of(cut) + [turns[1][2]] * bits_of(blocks)

    def settle(q, part):
        def body(t, carry):
            at = pl.ds(pl.multiple_of(t * 8, 8), 8)
            xs = mix_list([home[d, q, part, at] for d in range(n)], own_turns)
            for d in range(n):
                if q < parts - 1:
                    home[d, q, part, at] = xs[d]
                    continue
                ys = [home[d, r, part, at] for r in range(q)] + [xs[d]]
                ys = mix_list(ys, [turns[1][1]] * bits_of(parts))
                b, p = d // cut, d % cut
                for r in range(parts):
                    k = (d.bit_count() + r.bit_count() - part) % 4
                    y = -ys[r] if k in (1, 2) else ys[r]
                    out[k % 2, b, pl.ds(pl.multiple_of(p * rp + r * rq + t * 8, 8), 8)] = y
            return carry
        lax.fori_loop(0, rq // 8, body, 0)

    for i, (q, part, count) in enumerate(pieces):
        wait_all(lambda d: piece_of(home, d, i), ret_recv.at[i])
        for j in range(count):
            settle(q, part + j)
    for i in range(len(pieces)):
        wait_all(lambda d: piece_of(back, d, i), ret_send.at[i])


def put_out(done, out, sem):
    blocks = done.shape[1]
    copies = []
    for part in range(2):
        for q in range(2):
            at = pl.ds(q * (blocks // 2), blocks // 2)
            copies.append(pltpu.make_async_copy(done.at[part, at], out.at[part, at], sem.at[2 * part + q]))
    for copy in copies:
        copy.start()
    for copy in copies:
        copy.wait()


def solution(mesh):
    nh, nl = mesh.shape["high"], mesh.shape["low"]
    n = nh * nl

    def on_device(wave, level, diag, turn):
        blocks, rows, lanes = level.shape
        rp = rows // (n // blocks)
        parts = 2 if rp % 16 == 0 else 1
        hbm = pl.BlockSpec(memory_space=pltpu.HBM)
        dma = pltpu.SemaphoreType.DMA
        done = pl.pallas_call(
            functools.partial(kernel, nh, nl, parts),
            out_shape=pltpu.VMEM(wave.shape, F32),
            in_specs=[hbm] * 4,
            out_specs=pl.BlockSpec(memory_space=pltpu.VMEM),
            scratch_shapes=[
                pltpu.VMEM(diag.shape, F32),
                pltpu.SMEM(turn.shape, F32),
                pltpu.VMEM(wave.shape, F32),
                pltpu.VMEM(level.shape, F32),
                pltpu.VMEM((n, parts, 2 * rp // parts, lanes), F32),
                pltpu.VMEM((n, parts, 2 * rp // parts, lanes), F32),
                pltpu.VMEM((n, rp, lanes), F32),
                pltpu.VMEM((n, parts, 2, rp // parts, lanes), F32),
                pltpu.VMEM((n, parts, 2, rp // parts, lanes), F32),
                pltpu.VMEM((2, 2 * lanes, 2 * lanes), BF16),
                pltpu.VMEM((2, 2 * rows, 2 * rows), BF16),
                dma((4,)), pltpu.SemaphoreType.REGULAR, dma, dma, dma((parts,)), dma((parts,)),
                dma((parts + 1,)), dma((parts + 1,)),
            ],
            compiler_params=pltpu.CompilerParams(
                collective_id=0, has_side_effects=True, vmem_limit_bytes=20 * 2**20),
        )(*[pltpu.with_memory_space_constraint(x, pltpu.HBM) for x in (wave, level, diag, turn)])
        return pl.pallas_call(
            put_out,
            out_shape=jax.ShapeDtypeStruct(wave.shape, F32),
            in_specs=[pl.BlockSpec(memory_space=pltpu.VMEM)],
            out_specs=hbm,
            scratch_shapes=[dma((4,))],
            compiler_params=pltpu.CompilerParams(vmem_limit_bytes=2**20),
        )(done)

    in_specs = (P(None, ("high", "low"), None, None), P(("high", "low"), None, None), P(), P())
    return jax.shard_map(
        on_device, mesh=mesh, in_specs=in_specs,
        out_specs=P(None, ("high", "low"), None, None), check_vma=False)
```

```python
import functools

import jax
import jax.numpy as jnp
import numpy as np
from jax import lax
from jax.experimental import pallas as pl
from jax.experimental.pallas import tpu as pltpu
from jax.sharding import PartitionSpec as P

MESH = pl.DeviceIdType.MESH
F32 = jnp.float32
BF16 = jnp.bfloat16


def fit(function, powers, reach=3.2):
    x = np.cos(np.pi * (np.arange(4000) + 0.5) / 4000) * reach
    scaled = np.stack([(x / reach) ** p for p in powers], 1)
    found = np.linalg.lstsq(scaled, function(x), rcond=None)[0]
    return [float(f / reach**p) for f, p in zip(found, powers)]


SIN = fit(np.sin, range(1, 16, 2))
COS = fit(np.cos, range(0, 17, 2))


def cos_sin(x):
    z = x * x
    sine = jnp.full_like(x, SIN[-1])
    for f in SIN[-2::-1]:
        sine = sine * z + f
    cosine = jnp.full_like(x, COS[-1])
    for f in COS[-2::-1]:
        cosine = cosine * z + f
    return cosine, sine * x


def bits_of(count):
    return count.bit_length() - 1


def pop(values, bits):
    total = values % 2
    for q in range(1, bits):
        total = total + (values // 2**q) % 2
    return total


def pop_array(values, bits):
    total = values & 1
    for q in range(1, bits):
        total = total + ((values >> q) & 1)
    return total


def mix_list(xs, turns):
    for q, (c, s) in enumerate(turns):
        step = 1 << q
        ys = list(xs)
        for i in range(len(xs)):
            if not i & step:
                u, v = xs[i], xs[i + step]
                ys[i] = c * u - s * v
                ys[i + step] = s * u + c * v
        xs = ys
    return xs


def rotation(count, c, s, transposed, mixed):
    i = lax.broadcasted_iota(jnp.int32, (count, count), 0)
    j = lax.broadcasted_iota(jnp.int32, (count, count), 1)
    if transposed:
        i, j = j, i
    c, s = c[:1, :count], s[:1, :count]
    table = jnp.where((i >> mixed) == (j >> mixed), 1.0, 0.0)
    for q in range(mixed):
        a, b = (i >> q) & 1, (j >> q) & 1
        table = table * jnp.where(a == b, c, jnp.where(a == 1, s, -s))
    return table


def split(x):
    hi = x.astype(BF16)
    return hi, (x - hi.astype(F32)).astype(BF16)


def kernel(nh, nl, parts, wave_hbm, level_hbm, diag_hbm, turn_hbm, out,
           diag, turn, wave, level, relay, abuf, recv, lev, back, home, lane_t, row_t,
           in_sem, ready, relay_send, relay_recv, lev_send, lev_recv, to_send, to_recv, ret_send, ret_recv):
    n = nh * nl
    rp, lanes = level.shape[-2:]
    blocks, rows = wave.shape[1:3]
    cut = n // blocks
    rq = rp // parts
    h, l = lax.axis_index("high"), lax.axis_index("low")
    me = h * nl + l

    quad = nl // 4
    half = nl // 2

    zi, yi = l // quad, l % quad
    side = zi // 2
    partner = h * nl + (l ^ (3 * quad))
    directions = [(1 << i, 0) for i in range(bits_of(nh))] + [(0, 1 << i) for i in range(bits_of(quad))]
    directions += [(0, quad), (0, 3 * quad)]

    def call(body, dh, dl):
        body(dh * nl + dl, (dh, dl))

    def far_line(j):
        return jnp.where(zi < 2, 3 - j, j) * quad

    def far(body):
        def step(k, carry):
            t = k // nh
            call(body, h ^ (nh - 1 - k % nh), far_line(t // quad) + (yi ^ (quad - 1 - t % quad)))
            return carry
        lax.fori_loop(0, n // 2, step, 0)

    def near(body):
        def step(k, carry):
            call(body, h ^ (nh - 1 - k % nh), l ^ (half - 1 - k // nh))
            return carry
        lax.fori_loop(0, n // 2 - 1, step, 0)

    def others(body):
        near(body)
        far(body)

    def level_in(which, i):
        return pltpu.make_async_copy(level_hbm.at[:, which], level.at[:, which], in_sem.at[i])

    wave_in = pltpu.make_async_copy(wave_hbm, wave, in_sem.at[1])
    diag_in = pltpu.make_async_copy(diag_hbm, diag, in_sem.at[2])
    turn_in = pltpu.make_async_copy(turn_hbm, turn, in_sem.at[3])
    level_in(1 - side, 0).start()
    level_in(side, 4).start()
    turn_in.start()
    diag_in.start()
    wave_in.start()

    barrier = pltpu.get_barrier_semaphore()

    def greet(sem):
        return lambda d, at: pl.semaphore_signal(sem, inc=1, device_id=at, device_id_type=MESH)

    for dh, dl in directions:
        call(greet(barrier), h ^ dh, l ^ dl)
    level_in(1 - side, 0).wait()
    pl.semaphore_wait(barrier, len(directions))

    relay_copy = pltpu.make_async_remote_copy(
        src_ref=level.at[:, 1 - side], dst_ref=relay, send_sem=relay_send, recv_sem=relay_recv,
        device_id=(h, l ^ (3 * quad)), device_id_type=MESH)
    relay_copy.start()
    for i, (dh, dl) in enumerate(directions[1:]):
        call(greet(ready.at[i]), h ^ dh, l ^ dl)
        pl.semaphore_wait(ready.at[i], 1)
    level_in(side, 4).wait()

    def level_copy(d, at):
        return pltpu.make_async_remote_copy(
            src_ref=level.at[at[0], side, at[1] % half], dst_ref=lev.at[me],
            send_sem=lev_send, recv_sem=lev_recv,
            device_id=at, device_id_type=MESH)

    def pass_copy(d, at):
        return pltpu.make_async_remote_copy(
            src_ref=relay.at[at[0], at[1] % half], dst_ref=lev.at[partner],
            send_sem=lev_send, recv_sem=lev_recv,
            device_id=at, device_id_type=MESH)

    def to_copy(q):
        return lambda d, at: pltpu.make_async_remote_copy(
            src_ref=abuf.at[d, q], dst_ref=recv.at[me, q], send_sem=to_send.at[q],
            recv_sem=to_recv.at[q], device_id=at, device_id_type=MESH)

    pieces = [(q, 0, 2) for q in range(parts - 1)] + [(parts - 1, 0, 1), (parts - 1, 1, 1)]

    def piece_of(buf, d, i):
        q, part, count = pieces[i]
        return buf.at[d, q, pl.ds(part, count)]

    def ret_copy(i):
        return lambda d, at: pltpu.make_async_remote_copy(
            src_ref=piece_of(back, d, i), dst_ref=piece_of(home, me, i),
            send_sem=ret_send.at[i], recv_sem=ret_recv.at[i],
            device_id=at, device_id_type=MESH)

    def wait_all(blocks_of, sem, count=n - 1):
        most = blocks_of(pl.ds(0, count))
        pltpu.make_async_copy(most, most, sem).wait()

    def start(copy):
        return lambda d, at: copy(d, at).start()

    near(start(level_copy))

    turn_in.wait()
    diag_in.wait()

    turns = []
    for layer in range(2):
        turns.append([cos_sin(jnp.full((8, lanes), turn[layer, g], F32)) for g in range(4)])
        c, s = turns[layer][0]
        hi, lo = split(rotation(lanes, c, s, True, bits_of(lanes)))
        lane_t[layer] = jnp.concatenate(
            [jnp.concatenate([hi, lo], 1), jnp.concatenate([hi, jnp.zeros_like(hi)], 1)], 0)
        c, s = turns[layer][1]
        hi, lo = split(rotation(rows, c, s, False, bits_of(rows if layer == 0 else rq)))
        row_t[layer] = jnp.concatenate(
            [jnp.concatenate([hi, hi], 1), jnp.concatenate([lo, jnp.zeros_like(hi)], 1)], 0)

    ones = pop_array(lax.broadcasted_iota(jnp.int32, (rows, lanes), 0), bits_of(rows)) + pop_array(
        lax.broadcasted_iota(jnp.int32, (rows, lanes), 1), bits_of(lanes))
    ones_dev = pop(me, bits_of(n))

    def mix_lanes(x, layer):
        hi, lo = split(x)
        z = jnp.dot(jnp.concatenate([hi, lo], 1), lane_t[layer], preferred_element_type=F32)
        return z[:, :lanes] + z[:, lanes:]

    def mix_rows(x, y, layer):
        hi, lo = split(jnp.concatenate([x, y], 1))
        z = jnp.dot(row_t[layer], jnp.concatenate([hi, lo], 0), preferred_element_type=F32)
        z = z[:rows] + z[rows:]
        return z[:, :lanes], z[:, lanes:]

    def mix_blocks(buf, middle_at, start, count, layer):
        pair = [turns[layer][2]] * bits_of(blocks)
        per = count // 8

        def body(t, carry):
            p, at = t // per, pl.ds(pl.multiple_of(start + (t % per) * 8, 8), 8)
            xs = mix_list([buf[b * cut + p, middle_at, at] for b in range(blocks)], pair)
            for b in range(blocks):
                buf[b * cut + p, middle_at, at] = xs[b]
            return carry
        lax.fori_loop(0, cut * per, body, 0)

    def quarter(count):
        k = (ones + count) & 3
        return (k & 1) == 1, jnp.where(k >= 2, -1.0, 1.0)

    wave_in.wait()
    lev[me] = level[h, side, l % half]

    def first(b, carry):
        slots = [b * cut + p for p in range(cut)]
        e = jnp.concatenate([level[d // nl, d % nl // half, d % half] for d in slots], 0)
        c, s = cos_sin(e * diag[pl.ds(0, 1), :])
        odd, sign = quarter(ones_dev + pop(b, bits_of(blocks)))
        cc = jnp.where(odd, s, c) * sign
        ss = jnp.where(odd, -c, s) * sign
        re, im = wave[0, b], wave[1, b]
        z = mix_lanes(jnp.concatenate([re * cc + im * ss, im * cc - re * ss], 0), 0)
        re, im = mix_rows(z[:rows], z[rows:], 0)
        for p in range(cut):
            for q in range(parts):
                at = p * rp + q * rq
                abuf[b * cut + p, q, :rq] = re[at:at + rq]
                abuf[b * cut + p, q, rq:] = im[at:at + rq]
        return carry
    lax.fori_loop(0, blocks, first, 0)
    for q in range(parts):
        mix_blocks(abuf, q, 0, 2 * rq, 0)
        others(start(to_copy(q)))
        recv[me, q] = abuf[me, q]
        if q == 0:
            relay_copy.wait_recv()
            near(start(pass_copy))
            lev[partner] = relay[h, l % half]

    def dev_turns(layer):
        return [turns[layer][3]] * bits_of(nl) + [turns[layer][2]] * bits_of(nh)

    def middle(q):
        def body(j, carry):
            at = pl.ds(pl.multiple_of(j * 8, 8), 8)
            at_im = pl.ds(pl.multiple_of(rq + j * 8, 8), 8)
            at_part = pl.ds(pl.multiple_of(q * rq + j * 8, 8), 8)
            xs = mix_list([recv[d, q, at] for d in range(n)], dev_turns(0))
            for d in range(n):
                recv[d, q, at] = xs[d]
            ys = mix_list([recv[d, q, at_im] for d in range(n)], dev_turns(0))
            angle = diag[pl.ds(1, 1), :]
            for d in range(n):
                c, s = cos_sin(lev[d, at_part] * angle)
                x, y = recv[d, q, at], ys[d]
                recv[d, q, at] = x * c + y * s
                ys[d] = y * c - x * s
            ys = mix_list(ys, dev_turns(1))
            for d in range(n):
                back[d, q, 1, at] = ys[d]
            xs = mix_list([recv[d, q, at] for d in range(n)], dev_turns(1))
            for d in range(n):
                back[d, q, 0, at] = xs[d]
            return carry
        lax.fori_loop(0, rq // 8, body, 0)

    group = rows // rq

    def finish(q):
        def body(i, carry):
            ds = pl.ds(i * group, group)
            z = [back[ds, q, part].reshape(rows, lanes) for part in range(2)]
            z = mix_lanes(jnp.concatenate(z, 0), 1)
            re, im = mix_rows(z[:rows], z[rows:], 1)
            odd, sign = quarter(pop(i, bits_of(n // group)))
            back[ds, q, 0] = (jnp.where(odd, im, re) * sign).reshape(group, rq, lanes)
            back[ds, q, 1] = (jnp.where(odd, -re, im) * sign).reshape(group, rq, lanes)
            return carry
        lax.fori_loop(0, n // group, body, 0, unroll=2)

    wait_all(lambda d: lev.at[d], lev_recv, n - 2)
    for q in range(parts):
        wait_all(lambda d: recv.at[d, q], to_recv.at[q])
        middle(q)
        finish(q)
        for i, piece in enumerate(pieces):
            if piece[0] == q:
                others(start(ret_copy(i)))
    home[me] = back[me]

    relay_copy.wait_send()
    wait_all(lambda d: lev.at[d], lev_send, n - 2)
    for q in range(parts):
        wait_all(lambda d: abuf.at[d, q], to_send.at[q])

    own_turns = [turns[1][1]] * bits_of(cut) + [turns[1][2]] * bits_of(blocks)

    def settle(q, part):
        def body(t, carry):
            at = pl.ds(pl.multiple_of(t * 8, 8), 8)
            xs = mix_list([home[d, q, part, at] for d in range(n)], own_turns)
            for d in range(n):
                if q < parts - 1:
                    home[d, q, part, at] = xs[d]
                    continue
                ys = [home[d, r, part, at] for r in range(q)] + [xs[d]]
                ys = mix_list(ys, [turns[1][1]] * bits_of(parts))
                b, p = d // cut, d % cut
                for r in range(parts):
                    k = (d.bit_count() + r.bit_count() - part) % 4
                    y = -ys[r] if k in (1, 2) else ys[r]
                    out[k % 2, b, pl.ds(pl.multiple_of(p * rp + r * rq + t * 8, 8), 8)] = y
            return carry
        lax.fori_loop(0, rq // 8, body, 0)

    for i, (q, part, count) in enumerate(pieces):
        wait_all(lambda d: piece_of(home, d, i), ret_recv.at[i])
        for j in range(count):
            settle(q, part + j)
    for i in range(len(pieces)):
        wait_all(lambda d: piece_of(back, d, i), ret_send.at[i])


def put_out(done, out, sem):
    blocks = done.shape[1]
    copies = []
    for part in range(2):
        for q in range(2):
            at = pl.ds(q * (blocks // 2), blocks // 2)
            copies.append(pltpu.make_async_copy(done.at[part, at], out.at[part, at], sem.at[2 * part + q]))
    for copy in copies:
        copy.start()
    for copy in copies:
        copy.wait()


def solution(mesh):
    nh, nl = mesh.shape["high"], mesh.shape["low"]
    n = nh * nl

    def on_device(wave, level, diag, turn):
        blocks, rows, lanes = level.shape
        rp = rows // (n // blocks)
        level = level.reshape(nh, 2, nl // 2, rp, lanes)
        parts = 2 if rp % 16 == 0 else 1
        hbm = pl.BlockSpec(memory_space=pltpu.HBM)
        dma = pltpu.SemaphoreType.DMA
        done = pl.pallas_call(
            functools.partial(kernel, nh, nl, parts),
            out_shape=pltpu.VMEM(wave.shape, F32),
            in_specs=[hbm] * 4,
            out_specs=pl.BlockSpec(memory_space=pltpu.VMEM),
            scratch_shapes=[
                pltpu.VMEM(diag.shape, F32),
                pltpu.SMEM(turn.shape, F32),
                pltpu.VMEM(wave.shape, F32),
                pltpu.VMEM(level.shape, F32),
                pltpu.VMEM((nh, nl // 2, rp, lanes), F32),
                pltpu.VMEM((n, parts, 2 * rp // parts, lanes), F32),
                pltpu.VMEM((n, parts, 2 * rp // parts, lanes), F32),
                pltpu.VMEM((n, rp, lanes), F32),
                pltpu.VMEM((n, parts, 2, rp // parts, lanes), F32),
                pltpu.VMEM((n, parts, 2, rp // parts, lanes), F32),
                pltpu.VMEM((2, 2 * lanes, 2 * lanes), BF16),
                pltpu.VMEM((2, 2 * rows, 2 * rows), BF16),
                dma((5,)), pltpu.SemaphoreType.REGULAR((bits_of(n),)), dma, dma, dma, dma, dma((parts,)), dma((parts,)),
                dma((parts + 1,)), dma((parts + 1,)),
            ],
            compiler_params=pltpu.CompilerParams(
                collective_id=0, has_side_effects=True, vmem_limit_bytes=20 * 2**20),
        )(*[pltpu.with_memory_space_constraint(x, pltpu.HBM) for x in (wave, level, diag, turn)])
        return pl.pallas_call(
            put_out,
            out_shape=jax.ShapeDtypeStruct(wave.shape, F32),
            in_specs=[pl.BlockSpec(memory_space=pltpu.VMEM)],
            out_specs=hbm,
            scratch_shapes=[dma((4,))],
            compiler_params=pltpu.CompilerParams(vmem_limit_bytes=2**20),
        )(done)

    in_specs = (P(None, ("high", "low"), None, None), P(("high", "low"), None, None), P(), P())
    return jax.shard_map(
        on_device, mesh=mesh, in_specs=in_specs,
        out_specs=P(None, ("high", "low"), None, None), check_vma=False)
```

```python
import functools

import jax
import jax.numpy as jnp
import numpy as np
from jax import lax
from jax.experimental import pallas as pl
from jax.experimental.pallas import tpu as pltpu
from jax.sharding import PartitionSpec as P

MESH = pl.DeviceIdType.MESH
F32 = jnp.float32
BF16 = jnp.bfloat16


def fit(function, powers, reach=3.2):
    x = np.cos(np.pi * (np.arange(4000) + 0.5) / 4000) * reach
    scaled = np.stack([(x / reach) ** p for p in powers], 1)
    found = np.linalg.lstsq(scaled, function(x), rcond=None)[0]
    return [float(f / reach**p) for f, p in zip(found, powers)]


SIN = fit(np.sin, range(1, 16, 2))
COS = fit(np.cos, range(0, 17, 2))


def cos_sin(x):
    z = x * x
    sine = jnp.full_like(x, SIN[-1])
    for f in SIN[-2::-1]:
        sine = sine * z + f
    cosine = jnp.full_like(x, COS[-1])
    for f in COS[-2::-1]:
        cosine = cosine * z + f
    return cosine, sine * x


def bits_of(count):
    return count.bit_length() - 1


def pop(values, bits):
    total = values % 2
    for q in range(1, bits):
        total = total + (values // 2**q) % 2
    return total


def pop_array(values, bits):
    total = values & 1
    for q in range(1, bits):
        total = total + ((values >> q) & 1)
    return total


def mix_list(xs, turns):
    for q, (c, s) in enumerate(turns):
        step = 1 << q
        ys = list(xs)
        for i in range(len(xs)):
            if not i & step:
                u, v = xs[i], xs[i + step]
                ys[i] = c * u - s * v
                ys[i + step] = s * u + c * v
        xs = ys
    return xs


def rotation(count, c, s, transposed, mixed):
    i = lax.broadcasted_iota(jnp.int32, (count, count), 0)
    j = lax.broadcasted_iota(jnp.int32, (count, count), 1)
    if transposed:
        i, j = j, i
    c, s = c[:1, :count], s[:1, :count]
    table = jnp.where((i >> mixed) == (j >> mixed), 1.0, 0.0)
    for q in range(mixed):
        a, b = (i >> q) & 1, (j >> q) & 1
        table = table * jnp.where(a == b, c, jnp.where(a == 1, s, -s))
    return table


def split(x):
    hi = x.astype(BF16)
    return hi, (x - hi.astype(F32)).astype(BF16)


def kernel(nh, nl, parts, wave_hbm, level_hbm, diag_hbm, turn_hbm, out,
           diag, turn, wave, level, relay, abuf, recv, lev, back, home, lane_t, row_t,
           in_sem, reply, ready, relay_send, relay_recv, lev_send, lev_recv, to_send, to_recv, ret_send, ret_recv):
    n = nh * nl
    rp, lanes = level.shape[-2:]
    blocks, rows = wave.shape[1:3]
    cut = n // blocks
    rq = rp // parts
    h, l = lax.axis_index("high"), lax.axis_index("low")
    me = h * nl + l

    quad = nl // 4
    half = nl // 2

    zi, yi = l // quad, l % quad
    side = zi // 2
    partner = h * nl + (l ^ (3 * quad))
    edges = [(1 << i, 0, (h >> i) & 1) for i in range(bits_of(nh))]
    edges += [(0, 1 << i, (l >> i) & 1) for i in range(bits_of(quad))]
    edges += [(0, quad, zi % 2)]

    def call(body, dh, dl):
        body(dh * nl + dl, (dh, dl))

    def far_line(j):
        return jnp.where(zi < 2, 3 - j, j) * quad

    def far(body):
        def step(k, carry):
            t = k // nh
            call(body, h ^ (nh - 1 - k % nh), far_line(t // quad) + (yi ^ (quad - 1 - t % quad)))
            return carry
        lax.fori_loop(0, n // 2, step, 0)

    def near(body):
        def step(k, carry):
            call(body, h ^ (nh - 1 - k % nh), l ^ (half - 1 - k // nh))
            return carry
        lax.fori_loop(0, n // 2 - 1, step, 0)

    def others(body):
        near(body)
        far(body)

    barrier = pltpu.get_barrier_semaphore()

    def greet(sem):
        return lambda d, at: pl.semaphore_signal(sem, inc=1, device_id=at, device_id_type=MESH)

    def wait_reply(i):
        @pl.when(edges[i][2] == 0)
        def _():
            pl.semaphore_wait(reply.at[i], 1)

    call(greet(barrier), h, l ^ (3 * quad))
    for dh, dl, upper in edges:
        @pl.when(upper == 0)
        def _():
            call(greet(barrier), h ^ dh, l ^ dl)

    def level_in(which, i):
        return pltpu.make_async_copy(level_hbm.at[:, which], level.at[:, which], in_sem.at[i])

    wave_in = pltpu.make_async_copy(wave_hbm, wave, in_sem.at[1])
    diag_in = pltpu.make_async_copy(diag_hbm, diag, in_sem.at[2])
    turn_in = pltpu.make_async_copy(turn_hbm, turn, in_sem.at[3])
    level_in(1 - side, 0).start()
    level_in(side, 4).start()
    turn_in.start()
    diag_in.start()
    wave_in.start()

    pl.semaphore_wait(barrier, sum(upper for _, _, upper in edges) + 1)

    relay_copy = pltpu.make_async_remote_copy(
        src_ref=level_hbm.at[:, 1 - side], dst_ref=relay, send_sem=relay_send, recv_sem=relay_recv,
        device_id=(h, l ^ (3 * quad)), device_id_type=MESH)
    relay_copy.start()
    for i, (dh, dl, upper) in enumerate(edges):
        @pl.when(upper == 1)
        def _():
            call(greet(reply.at[i]), h ^ dh, l ^ dl)
    for i in range(len(edges)):
        wait_reply(i)
    for i, (dh, dl) in enumerate([edge[:2] for edge in edges[1:]] + [(0, 3 * quad)]):
        call(greet(ready.at[i]), h ^ dh, l ^ dl)
        pl.semaphore_wait(ready.at[i], 1)
    level_in(side, 4).wait()
    level_in(1 - side, 0).wait()

    def level_copy(d, at):
        return pltpu.make_async_remote_copy(
            src_ref=level.at[at[0], side, at[1] % half], dst_ref=lev.at[me],
            send_sem=lev_send, recv_sem=lev_recv,
            device_id=at, device_id_type=MESH)

    def pass_copy(d, at):
        return pltpu.make_async_remote_copy(
            src_ref=relay.at[at[0], at[1] % half], dst_ref=lev.at[partner],
            send_sem=lev_send, recv_sem=lev_recv,
            device_id=at, device_id_type=MESH)

    def to_copy(q):
        return lambda d, at: pltpu.make_async_remote_copy(
            src_ref=abuf.at[d, q], dst_ref=recv.at[me, q], send_sem=to_send.at[q],
            recv_sem=to_recv.at[q], device_id=at, device_id_type=MESH)

    pieces = [(q, 0, 2) for q in range(parts - 1)] + [(parts - 1, 0, 1), (parts - 1, 1, 1)]

    def piece_of(buf, d, i):
        q, part, count = pieces[i]
        return buf.at[d, q, pl.ds(part, count)]

    def ret_copy(i):
        return lambda d, at: pltpu.make_async_remote_copy(
            src_ref=piece_of(back, d, i), dst_ref=piece_of(home, me, i),
            send_sem=ret_send.at[i], recv_sem=ret_recv.at[i],
            device_id=at, device_id_type=MESH)

    def wait_all(blocks_of, sem, count=n - 1):
        most = blocks_of(pl.ds(0, count))
        pltpu.make_async_copy(most, most, sem).wait()

    def start(copy):
        return lambda d, at: copy(d, at).start()

    near(start(level_copy))

    turn_in.wait()
    diag_in.wait()

    turns = []
    for layer in range(2):
        turns.append([cos_sin(jnp.full((8, lanes), turn[layer, g], F32)) for g in range(4)])
        c, s = turns[layer][0]
        hi, lo = split(rotation(lanes, c, s, True, bits_of(lanes)))
        lane_t[layer] = jnp.concatenate(
            [jnp.concatenate([hi, lo], 1), jnp.concatenate([hi, jnp.zeros_like(hi)], 1)], 0)
        c, s = turns[layer][1]
        hi, lo = split(rotation(rows, c, s, False, bits_of(rows if layer == 0 else rq)))
        row_t[layer] = jnp.concatenate(
            [jnp.concatenate([hi, hi], 1), jnp.concatenate([lo, jnp.zeros_like(hi)], 1)], 0)

    ones = pop_array(lax.broadcasted_iota(jnp.int32, (rows, lanes), 0), bits_of(rows)) + pop_array(
        lax.broadcasted_iota(jnp.int32, (rows, lanes), 1), bits_of(lanes))
    ones_dev = pop(me, bits_of(n))

    def mix_lanes(x, layer):
        hi, lo = split(x)
        z = jnp.dot(jnp.concatenate([hi, lo], 1), lane_t[layer], preferred_element_type=F32)
        return z[:, :lanes] + z[:, lanes:]

    def mix_rows(x, y, layer):
        hi, lo = split(jnp.concatenate([x, y], 1))
        z = jnp.dot(row_t[layer], jnp.concatenate([hi, lo], 0), preferred_element_type=F32)
        z = z[:rows] + z[rows:]
        return z[:, :lanes], z[:, lanes:]

    def mix_blocks(buf, middle_at, start, count, layer):
        pair = [turns[layer][2]] * bits_of(blocks)
        per = count // 8

        def body(t, carry):
            p, at = t // per, pl.ds(pl.multiple_of(start + (t % per) * 8, 8), 8)
            xs = mix_list([buf[b * cut + p, middle_at, at] for b in range(blocks)], pair)
            for b in range(blocks):
                buf[b * cut + p, middle_at, at] = xs[b]
            return carry
        lax.fori_loop(0, cut * per, body, 0)

    def quarter(count):
        k = (ones + count) & 3
        return (k & 1) == 1, jnp.where(k >= 2, -1.0, 1.0)

    wave_in.wait()
    lev[me] = level[h, side, l % half]

    def first(b, carry):
        slots = [b * cut + p for p in range(cut)]
        e = jnp.concatenate([level[d // nl, d % nl // half, d % half] for d in slots], 0)
        c, s = cos_sin(e * diag[pl.ds(0, 1), :])
        odd, sign = quarter(ones_dev + pop(b, bits_of(blocks)))
        cc = jnp.where(odd, s, c) * sign
        ss = jnp.where(odd, -c, s) * sign
        re, im = wave[0, b], wave[1, b]
        z = mix_lanes(jnp.concatenate([re * cc + im * ss, im * cc - re * ss], 0), 0)
        re, im = mix_rows(z[:rows], z[rows:], 0)
        for p in range(cut):
            for q in range(parts):
                at = p * rp + q * rq
                abuf[b * cut + p, q, :rq] = re[at:at + rq]
                abuf[b * cut + p, q, rq:] = im[at:at + rq]
        return carry
    lax.fori_loop(0, blocks, first, 0)
    for q in range(parts):
        mix_blocks(abuf, q, 0, 2 * rq, 0)
        others(start(to_copy(q)))
        recv[me, q] = abuf[me, q]
        if q == 0:
            relay_copy.wait_recv()
            near(start(pass_copy))
            lev[partner] = relay[h, l % half]

    def dev_turns(layer):
        return [turns[layer][3]] * bits_of(nl) + [turns[layer][2]] * bits_of(nh)

    def middle(q):
        def body(j, carry):
            at = pl.ds(pl.multiple_of(j * 8, 8), 8)
            at_im = pl.ds(pl.multiple_of(rq + j * 8, 8), 8)
            at_part = pl.ds(pl.multiple_of(q * rq + j * 8, 8), 8)
            xs = mix_list([recv[d, q, at] for d in range(n)], dev_turns(0))
            for d in range(n):
                recv[d, q, at] = xs[d]
            ys = mix_list([recv[d, q, at_im] for d in range(n)], dev_turns(0))
            angle = diag[pl.ds(1, 1), :]
            for d in range(n):
                c, s = cos_sin(lev[d, at_part] * angle)
                x, y = recv[d, q, at], ys[d]
                recv[d, q, at] = x * c + y * s
                ys[d] = y * c - x * s
            ys = mix_list(ys, dev_turns(1))
            for d in range(n):
                back[d, q, 1, at] = ys[d]
            xs = mix_list([recv[d, q, at] for d in range(n)], dev_turns(1))
            for d in range(n):
                back[d, q, 0, at] = xs[d]
            return carry
        lax.fori_loop(0, rq // 8, body, 0)

    group = rows // rq

    def finish(q):
        def body(i, carry):
            ds = pl.ds(i * group, group)
            z = [back[ds, q, part].reshape(rows, lanes) for part in range(2)]
            z = mix_lanes(jnp.concatenate(z, 0), 1)
            re, im = mix_rows(z[:rows], z[rows:], 1)
            odd, sign = quarter(pop(i, bits_of(n // group)))
            back[ds, q, 0] = (jnp.where(odd, im, re) * sign).reshape(group, rq, lanes)
            back[ds, q, 1] = (jnp.where(odd, -re, im) * sign).reshape(group, rq, lanes)
            return carry
        lax.fori_loop(0, n // group, body, 0, unroll=2)

    wait_all(lambda d: lev.at[d], lev_recv, n - 2)
    for q in range(parts):
        wait_all(lambda d: recv.at[d, q], to_recv.at[q])
        middle(q)
        finish(q)
        for i, piece in enumerate(pieces):
            if piece[0] == q:
                others(start(ret_copy(i)))
    home[me] = back[me]

    relay_copy.wait_send()
    wait_all(lambda d: lev.at[d], lev_send, n - 2)
    for q in range(parts):
        wait_all(lambda d: abuf.at[d, q], to_send.at[q])

    own_turns = [turns[1][1]] * bits_of(cut) + [turns[1][2]] * bits_of(blocks)

    def settle(q, part):
        def body(t, carry):
            at = pl.ds(pl.multiple_of(t * 8, 8), 8)
            xs = mix_list([home[d, q, part, at] for d in range(n)], own_turns)
            for d in range(n):
                if q < parts - 1:
                    home[d, q, part, at] = xs[d]
                    continue
                ys = [home[d, r, part, at] for r in range(q)] + [xs[d]]
                ys = mix_list(ys, [turns[1][1]] * bits_of(parts))
                b, p = d // cut, d % cut
                for r in range(parts):
                    k = (d.bit_count() + r.bit_count() - part) % 4
                    y = -ys[r] if k in (1, 2) else ys[r]
                    out[k % 2, b, pl.ds(pl.multiple_of(p * rp + r * rq + t * 8, 8), 8)] = y
            return carry
        lax.fori_loop(0, rq // 8, body, 0)

    for i, (q, part, count) in enumerate(pieces):
        wait_all(lambda d: piece_of(home, d, i), ret_recv.at[i])
        for j in range(count):
            settle(q, part + j)
    for i in range(len(pieces)):
        wait_all(lambda d: piece_of(back, d, i), ret_send.at[i])


def put_out(done, out, sem):
    blocks = done.shape[1]
    copies = []
    for part in range(2):
        for q in range(2):
            at = pl.ds(q * (blocks // 2), blocks // 2)
            copies.append(pltpu.make_async_copy(done.at[part, at], out.at[part, at], sem.at[2 * part + q]))
    for copy in copies:
        copy.start()
    for copy in copies:
        copy.wait()


def solution(mesh):
    nh, nl = mesh.shape["high"], mesh.shape["low"]
    n = nh * nl

    def on_device(wave, level, diag, turn):
        blocks, rows, lanes = level.shape
        rp = rows // (n // blocks)
        level = level.reshape(nh, 2, nl // 2, rp, lanes)
        parts = 2 if rp % 16 == 0 else 1
        hbm = pl.BlockSpec(memory_space=pltpu.HBM)
        dma = pltpu.SemaphoreType.DMA
        done = pl.pallas_call(
            functools.partial(kernel, nh, nl, parts),
            out_shape=pltpu.VMEM(wave.shape, F32),
            in_specs=[hbm] * 4,
            out_specs=pl.BlockSpec(memory_space=pltpu.VMEM),
            scratch_shapes=[
                pltpu.VMEM(diag.shape, F32),
                pltpu.SMEM(turn.shape, F32),
                pltpu.VMEM(wave.shape, F32),
                pltpu.VMEM(level.shape, F32),
                pltpu.VMEM((nh, nl // 2, rp, lanes), F32),
                pltpu.VMEM((n, parts, 2 * rp // parts, lanes), F32),
                pltpu.VMEM((n, parts, 2 * rp // parts, lanes), F32),
                pltpu.VMEM((n, rp, lanes), F32),
                pltpu.VMEM((n, parts, 2, rp // parts, lanes), F32),
                pltpu.VMEM((n, parts, 2, rp // parts, lanes), F32),
                pltpu.VMEM((2, 2 * lanes, 2 * lanes), BF16),
                pltpu.VMEM((2, 2 * rows, 2 * rows), BF16),
                dma((5,)), *[pltpu.SemaphoreType.REGULAR((bits_of(n),))] * 2, dma, dma, dma, dma, dma((parts,)), dma((parts,)),
                dma((parts + 1,)), dma((parts + 1,)),
            ],
            compiler_params=pltpu.CompilerParams(
                collective_id=0, has_side_effects=True, vmem_limit_bytes=20 * 2**20),
        )(*[pltpu.with_memory_space_constraint(x, pltpu.HBM) for x in (wave, level, diag, turn)])
        return pl.pallas_call(
            put_out,
            out_shape=jax.ShapeDtypeStruct(wave.shape, F32),
            in_specs=[pl.BlockSpec(memory_space=pltpu.VMEM)],
            out_specs=hbm,
            scratch_shapes=[dma((4,))],
            compiler_params=pltpu.CompilerParams(vmem_limit_bytes=2**20),
        )(done)

    in_specs = (P(None, ("high", "low"), None, None), P(("high", "low"), None, None), P(), P())
    return jax.shard_map(
        on_device, mesh=mesh, in_specs=in_specs,
        out_specs=P(None, ("high", "low"), None, None), check_vma=False)
```

```python
import functools

import jax
import jax.numpy as jnp
import numpy as np
from jax import lax
from jax.experimental import pallas as pl
from jax.experimental.pallas import tpu as pltpu
from jax.sharding import PartitionSpec as P

MESH = pl.DeviceIdType.MESH
F32 = jnp.float32
BF16 = jnp.bfloat16


def fit(function, powers, reach=3.2):
    x = np.cos(np.pi * (np.arange(4000) + 0.5) / 4000) * reach
    scaled = np.stack([(x / reach) ** p for p in powers], 1)
    found = np.linalg.lstsq(scaled, function(x), rcond=None)[0]
    return [float(f / reach**p) for f, p in zip(found, powers)]


SIN = fit(np.sin, range(1, 16, 2))
COS = fit(np.cos, range(0, 17, 2))


def cos_sin(x):
    z = x * x
    sine = jnp.full_like(x, SIN[-1])
    for f in SIN[-2::-1]:
        sine = sine * z + f
    cosine = jnp.full_like(x, COS[-1])
    for f in COS[-2::-1]:
        cosine = cosine * z + f
    return cosine, sine * x


def bits_of(count):
    return count.bit_length() - 1


def pop(values, bits):
    total = values % 2
    for q in range(1, bits):
        total = total + (values // 2**q) % 2
    return total


def pop_array(values, bits):
    total = values & 1
    for q in range(1, bits):
        total = total + ((values >> q) & 1)
    return total


def mix_list(xs, turns):
    for q, (c, s) in enumerate(turns):
        step = 1 << q
        ys = list(xs)
        for i in range(len(xs)):
            if not i & step:
                u, v = xs[i], xs[i + step]
                ys[i] = c * u - s * v
                ys[i + step] = s * u + c * v
        xs = ys
    return xs


def mix_scaled(xs, tangents):
    for q, t in enumerate(tangents):
        step = 1 << q
        ys = list(xs)
        for i in range(len(xs)):
            if not i & step:
                u, v = xs[i], xs[i + step]
                ys[i] = u - t * v
                ys[i + step] = v + t * u
        xs = ys
    return xs


def rotation(count, c, s, transposed, mixed):
    i = lax.broadcasted_iota(jnp.int32, (count, count), 0)
    j = lax.broadcasted_iota(jnp.int32, (count, count), 1)
    if transposed:
        i, j = j, i
    c, s = c[:1, :count], s[:1, :count]
    table = jnp.where((i >> mixed) == (j >> mixed), 1.0, 0.0)
    for q in range(mixed):
        a, b = (i >> q) & 1, (j >> q) & 1
        table = table * jnp.where(a == b, c, jnp.where(a == 1, s, -s))
    return table


def split(x):
    hi = x.astype(BF16)
    return hi, (x - hi.astype(F32)).astype(BF16)


def kernel(nh, nl, parts, wave_hbm, level_hbm, diag_hbm, turn_hbm, home, tangent,
           diag, turn, wave, level, relay, abuf, recv, lev, back, lane_t, row_t,
           in_sem, reply, ready, relay_send, relay_recv, lev_send, lev_recv, to_send, to_recv, ret_send, ret_recv):
    n = nh * nl
    rp, lanes = level.shape[-2:]
    blocks, rows = wave.shape[1:3]
    cut = n // blocks
    rq = rp // parts
    h, l = lax.axis_index("high"), lax.axis_index("low")
    me = h * nl + l

    quad = nl // 4
    half = nl // 2

    zi, yi = l // quad, l % quad
    side = zi // 2
    partner = h * nl + (l ^ (3 * quad))
    edges = [(1 << i, 0, (h >> i) & 1) for i in range(bits_of(nh))]
    edges += [(0, 1 << i, (l >> i) & 1) for i in range(bits_of(quad))]
    edges += [(0, quad, zi % 2)]

    def call(body, dh, dl):
        body(dh * nl + dl, (dh, dl))

    def far_line(j):
        return jnp.where(zi < 2, 3 - j, j) * quad

    def far(body):
        def step(k, carry):
            t = k // nh
            call(body, h ^ (nh - 1 - k % nh), far_line(t // quad) + (yi ^ (quad - 1 - t % quad)))
            return carry
        lax.fori_loop(0, n // 2, step, 0)

    def near(body):
        def step(k, carry):
            call(body, h ^ (nh - 1 - k % nh), l ^ (half - 1 - k // nh))
            return carry
        lax.fori_loop(0, n // 2 - 1, step, 0)

    def others(body):
        near(body)
        far(body)

    barrier = pltpu.get_barrier_semaphore()

    def greet(sem):
        return lambda d, at: pl.semaphore_signal(sem, inc=1, device_id=at, device_id_type=MESH)

    def wait_reply(i):
        @pl.when(edges[i][2] == 0)
        def _():
            pl.semaphore_wait(reply.at[i], 1)

    call(greet(barrier), h, l ^ (3 * quad))
    for dh, dl, upper in edges:
        @pl.when(upper == 0)
        def _():
            call(greet(barrier), h ^ dh, l ^ dl)

    def level_in(which, i):
        return pltpu.make_async_copy(level_hbm.at[:, which], level.at[:, which], in_sem.at[i])

    wave_in = pltpu.make_async_copy(wave_hbm, wave, in_sem.at[1])
    diag_in = pltpu.make_async_copy(diag_hbm, diag, in_sem.at[2])
    turn_in = pltpu.make_async_copy(turn_hbm, turn, in_sem.at[3])
    level_in(1 - side, 0).start()
    level_in(side, 4).start()
    turn_in.start()
    diag_in.start()
    wave_in.start()

    pl.semaphore_wait(barrier, sum(upper for _, _, upper in edges) + 1)

    relay_copy = pltpu.make_async_remote_copy(
        src_ref=level_hbm.at[:, 1 - side], dst_ref=relay, send_sem=relay_send, recv_sem=relay_recv,
        device_id=(h, l ^ (3 * quad)), device_id_type=MESH)
    relay_copy.start()
    for i, (dh, dl, upper) in enumerate(edges):
        @pl.when(upper == 1)
        def _():
            call(greet(reply.at[i]), h ^ dh, l ^ dl)
    for i in range(len(edges)):
        wait_reply(i)
    for i, (dh, dl) in enumerate([edge[:2] for edge in edges[1:]] + [(0, 3 * quad)]):
        call(greet(ready.at[i]), h ^ dh, l ^ dl)
        pl.semaphore_wait(ready.at[i], 1)
    level_in(side, 4).wait()
    level_in(1 - side, 0).wait()

    def level_copy(d, at):
        return pltpu.make_async_remote_copy(
            src_ref=level.at[at[0], side, at[1] % half], dst_ref=lev.at[me],
            send_sem=lev_send, recv_sem=lev_recv,
            device_id=at, device_id_type=MESH)

    def pass_copy(d, at):
        return pltpu.make_async_remote_copy(
            src_ref=relay.at[at[0], at[1] % half], dst_ref=lev.at[partner],
            send_sem=lev_send, recv_sem=lev_recv,
            device_id=at, device_id_type=MESH)

    def to_copy(q):
        return lambda d, at: pltpu.make_async_remote_copy(
            src_ref=abuf.at[d, q], dst_ref=recv.at[me, q], send_sem=to_send.at[q],
            recv_sem=to_recv.at[q], device_id=at, device_id_type=MESH)

    pieces = [(q, 0, 2) for q in range(parts - 1)] + [(parts - 1, 0, 1), (parts - 1, 1, 1)]

    def piece_of(buf, d, i):
        q, part, count = pieces[i]
        return buf.at[d, q, pl.ds(part, count)]

    def ret_copy(i):
        return lambda d, at: pltpu.make_async_remote_copy(
            src_ref=piece_of(back, d, i), dst_ref=piece_of(home, me, i),
            send_sem=ret_send.at[i], recv_sem=ret_recv.at[i],
            device_id=at, device_id_type=MESH)

    def wait_all(blocks_of, sem, count=n - 1):
        most = blocks_of(pl.ds(0, count))
        pltpu.make_async_copy(most, most, sem).wait()

    def start(copy):
        return lambda d, at: copy(d, at).start()

    near(start(level_copy))

    turn_in.wait()
    diag_in.wait()

    turns = []
    for layer in range(2):
        turns.append([cos_sin(jnp.full((8, lanes), turn[layer, g], F32)) for g in range(4)])
        c, s = turns[layer][0]
        hi, lo = split(rotation(lanes, c, s, True, bits_of(lanes)))
        lane_t[layer] = jnp.concatenate(
            [jnp.concatenate([hi, lo], 1), jnp.concatenate([hi, jnp.zeros_like(hi)], 1)], 0)
        c, s = turns[layer][1]
        hi, lo = split(rotation(rows, c, s, False, bits_of(rows if layer == 0 else rq)))
        row_t[layer] = jnp.concatenate(
            [jnp.concatenate([hi, hi], 1), jnp.concatenate([lo, jnp.zeros_like(hi)], 1)], 0)

    ones = pop_array(lax.broadcasted_iota(jnp.int32, (rows, lanes), 0), bits_of(rows)) + pop_array(
        lax.broadcasted_iota(jnp.int32, (rows, lanes), 1), bits_of(lanes))
    ones_dev = pop(me, bits_of(n))

    def mix_lanes(x, layer):
        hi, lo = split(x)
        z = jnp.dot(jnp.concatenate([hi, lo], 1), lane_t[layer], preferred_element_type=F32)
        return z[:, :lanes] + z[:, lanes:]

    def mix_rows(x, y, layer):
        hi, lo = split(jnp.concatenate([x, y], 1))
        z = jnp.dot(row_t[layer], jnp.concatenate([hi, lo], 0), preferred_element_type=F32)
        z = z[:rows] + z[rows:]
        return z[:, :lanes], z[:, lanes:]

    def mix_blocks(buf, middle_at, start, count, layer):
        pair = [turns[layer][2]] * bits_of(blocks)
        per = count // 8

        def body(t, carry):
            p, at = t // per, pl.ds(pl.multiple_of(start + (t % per) * 8, 8), 8)
            xs = mix_list([buf[b * cut + p, middle_at, at] for b in range(blocks)], pair)
            for b in range(blocks):
                buf[b * cut + p, middle_at, at] = xs[b]
            return carry
        lax.fori_loop(0, cut * per, body, 0)

    def quarter(count):
        k = (ones + count) & 3
        return (k & 1) == 1, jnp.where(k >= 2, -1.0, 1.0)

    wave_in.wait()
    lev[me] = level[h, side, l % half]

    def first(b, carry):
        slots = [b * cut + p for p in range(cut)]
        e = jnp.concatenate([level[d // nl, d % nl // half, d % half] for d in slots], 0)
        c, s = cos_sin(e * diag[pl.ds(0, 1), :])
        odd, sign = quarter(ones_dev + pop(b, bits_of(blocks)))
        cc = jnp.where(odd, s, c) * sign
        ss = jnp.where(odd, -c, s) * sign
        re, im = wave[0, b], wave[1, b]
        z = mix_lanes(jnp.concatenate([re * cc + im * ss, im * cc - re * ss], 0), 0)
        re, im = mix_rows(z[:rows], z[rows:], 0)
        for p in range(cut):
            for q in range(parts):
                at = p * rp + q * rq
                abuf[b * cut + p, q, :rq] = re[at:at + rq]
                abuf[b * cut + p, q, rq:] = im[at:at + rq]
        return carry
    lax.fori_loop(0, blocks, first, 0)
    for q in range(parts):
        mix_blocks(abuf, q, 0, 2 * rq, 0)
        others(start(to_copy(q)))
        recv[me, q] = abuf[me, q]
        if q == 0:
            relay_copy.wait_recv()
            near(start(pass_copy))
            lev[partner] = relay[h, l % half]

    def dev_turns(layer):
        return [turns[layer][3]] * bits_of(nl) + [turns[layer][2]] * bits_of(nh)

    def middle(q):
        def body(j, carry):
            at = pl.ds(pl.multiple_of(j * 8, 8), 8)
            at_im = pl.ds(pl.multiple_of(rq + j * 8, 8), 8)
            at_part = pl.ds(pl.multiple_of(q * rq + j * 8, 8), 8)
            xs = mix_list([recv[d, q, at] for d in range(n)], dev_turns(0))
            for d in range(n):
                recv[d, q, at] = xs[d]
            ys = mix_list([recv[d, q, at_im] for d in range(n)], dev_turns(0))
            angle = diag[pl.ds(1, 1), :]
            for d in range(n):
                c, s = cos_sin(lev[d, at_part] * angle)
                x, y = recv[d, q, at], ys[d]
                recv[d, q, at] = x * c + y * s
                ys[d] = y * c - x * s
            ys = mix_list(ys, dev_turns(1))
            for d in range(n):
                back[d, q, 1, at] = ys[d]
            xs = mix_list([recv[d, q, at] for d in range(n)], dev_turns(1))
            for d in range(n):
                back[d, q, 0, at] = xs[d]
            return carry
        lax.fori_loop(0, rq // 8, body, 0)

    tangents = [turns[1][g][1] / turns[1][g][0] for g in (1, 2)]
    own_tangents = [tangents[0]] * bits_of(cut) + [tangents[1]] * bits_of(blocks)
    half_tangents = [tangents[0]] * bits_of(parts)
    tangent[0], tangent[1] = tangents
    scale = jnp.ones((1, lanes), F32)
    for g, count in ((1, bits_of(cut * parts)), (2, bits_of(blocks))):
        for _ in range(count):
            scale = scale * turns[1][g][0][:1]

    group = rows // rq

    def finish(q):
        def body(i, carry):
            ds = pl.ds(i * group, group)
            z = [back[ds, q, part].reshape(rows, lanes) for part in range(2)]
            z = mix_lanes(jnp.concatenate(z, 0), 1)
            re, im = mix_rows(z[:rows], z[rows:], 1)
            odd, sign = quarter(pop(i, bits_of(n // group)))
            sign = sign * scale
            back[ds, q, 0] = (jnp.where(odd, im, re) * sign).reshape(group, rq, lanes)
            back[ds, q, 1] = (jnp.where(odd, -re, im) * sign).reshape(group, rq, lanes)
            return carry
        lax.fori_loop(0, n // group, body, 0, unroll=2)

    wait_all(lambda d: lev.at[d], lev_recv, n - 2)
    for q in range(parts):
        wait_all(lambda d: recv.at[d, q], to_recv.at[q])
        middle(q)
        finish(q)
        for i, piece in enumerate(pieces):
            if piece[0] == q:
                others(start(ret_copy(i)))
    home[me] = back[me]

    relay_copy.wait_send()
    wait_all(lambda d: lev.at[d], lev_send, n - 2)
    for q in range(parts):
        wait_all(lambda d: abuf.at[d, q], to_send.at[q])

    def settle(q, part):
        def body(t, carry):
            at = pl.ds(pl.multiple_of(t * 8, 8), 8)
            xs = mix_scaled([home[d, q, part, at] for d in range(n)], own_tangents)
            for d in range(n):
                if q < parts - 1:
                    home[d, q, part, at] = xs[d]
                    continue
                ys = [home[d, r, part, at] for r in range(q)] + [xs[d]]
                ys = mix_scaled(ys, half_tangents)
                for r in range(parts):
                    home[d, r, part, at] = -ys[r] if place(d, r, part)[1] else ys[r]
            return carry
        lax.fori_loop(0, rq // 8, body, 0)

    for i, (q, part, count) in enumerate(pieces):
        wait_all(lambda d: piece_of(home, d, i), ret_recv.at[i])
        for j in range(count):
            if (q, part) != pieces[-1][:2]:
                settle(q, part + j)
    for i in range(len(pieces)):
        wait_all(lambda d: piece_of(back, d, i), ret_send.at[i])


def place(d, r, part):
    k = (d.bit_count() + r.bit_count() - part) % 4
    return k % 2, k in (1, 2)


def close(home, tangent, out_hbm, out, sem):
    n, parts, _, rq, lanes = home.shape
    blocks = out.shape[1]
    cut = n // blocks
    own_tangents = [tangent[0]] * bits_of(cut) + [tangent[1]] * bits_of(blocks)

    def out_copy(t):
        at = pl.ds(pl.multiple_of(t * 8, 8), 8)
        return pltpu.make_async_copy(
            out.at[:, :, :, :, at], out_hbm.at[:, :, :, :, at], sem.at[t])

    def body(t, carry):
        at = pl.ds(pl.multiple_of(t * 8, 8), 8)
        xs = mix_scaled([home[d, parts - 1, 1, at] for d in range(n)], own_tangents)
        for d in range(n):
            b, p = d // cut, d % cut
            ys = [home[d, r, 1, at] for r in range(parts - 1)] + [xs[d]]
            ys = mix_scaled(ys, [tangent[0]] * bits_of(parts))
            for r in range(parts):
                index, minus = place(d, r, 1)
                out[index, b, p, r, at] = -ys[r] if minus else ys[r]
                out[1 - index, b, p, r, at] = home[d, r, 0, at]
        out_copy(t).start()
        return carry
    lax.fori_loop(0, rq // 8, body, 0)
    for t in range(rq // 8):
        out_copy(t).wait()


def solution(mesh):
    nh, nl = mesh.shape["high"], mesh.shape["low"]
    n = nh * nl

    def on_device(wave, level, diag, turn):
        blocks, rows, lanes = level.shape
        rp = rows // (n // blocks)
        level = level.reshape(nh, 2, nl // 2, rp, lanes)
        parts = 2 if rp % 16 == 0 else 1
        hbm = pl.BlockSpec(memory_space=pltpu.HBM)
        vmem = pl.BlockSpec(memory_space=pltpu.VMEM)
        dma = pltpu.SemaphoreType.DMA
        home, tangent = pl.pallas_call(
            functools.partial(kernel, nh, nl, parts),
            out_shape=(pltpu.VMEM((n, parts, 2, rp // parts, lanes), F32), pltpu.VMEM((2, 8, lanes), F32)),
            in_specs=[hbm] * 4,
            out_specs=(vmem, vmem),
            scratch_shapes=[
                pltpu.VMEM(diag.shape, F32),
                pltpu.SMEM(turn.shape, F32),
                pltpu.VMEM(wave.shape, F32),
                pltpu.VMEM(level.shape, F32),
                pltpu.VMEM((nh, nl // 2, rp, lanes), F32),
                pltpu.VMEM((n, parts, 2 * rp // parts, lanes), F32),
                pltpu.VMEM((n, parts, 2 * rp // parts, lanes), F32),
                pltpu.VMEM((n, rp, lanes), F32),
                pltpu.VMEM((n, parts, 2, rp // parts, lanes), F32),
                pltpu.VMEM((2, 2 * lanes, 2 * lanes), BF16),
                pltpu.VMEM((2, 2 * rows, 2 * rows), BF16),
                dma((5,)), *[pltpu.SemaphoreType.REGULAR((bits_of(n),))] * 2, dma, dma, dma, dma, dma((parts,)), dma((parts,)),
                dma((parts + 1,)), dma((parts + 1,)),
            ],
            compiler_params=pltpu.CompilerParams(
                collective_id=0, has_side_effects=True, vmem_limit_bytes=20 * 2**20),
        )(*[pltpu.with_memory_space_constraint(x, pltpu.HBM) for x in (wave, level, diag, turn)])
        split_shape = (2, blocks, n // blocks, parts, rp // parts, lanes)
        out = pl.pallas_call(
            close,
            out_shape=jax.ShapeDtypeStruct(split_shape, F32),
            in_specs=[vmem, vmem],
            out_specs=hbm,
            scratch_shapes=[pltpu.VMEM(split_shape, F32), dma((rp // parts // 8,))],
            compiler_params=pltpu.CompilerParams(vmem_limit_bytes=8 * 2**20),
        )(home, tangent)
        return out.reshape(wave.shape)

    in_specs = (P(None, ("high", "low"), None, None), P(("high", "low"), None, None), P(), P())
    return jax.shard_map(
        on_device, mesh=mesh, in_specs=in_specs,
        out_specs=P(None, ("high", "low"), None, None), check_vma=False)
```

```python
import functools

import jax
import jax.numpy as jnp
import numpy as np
from jax import lax
from jax.experimental import pallas as pl
from jax.experimental.pallas import tpu as pltpu
from jax.sharding import PartitionSpec as P

MESH = pl.DeviceIdType.MESH
F32 = jnp.float32
BF16 = jnp.bfloat16


def fit(function, powers, reach=3.2):
    x = np.cos(np.pi * (np.arange(4000) + 0.5) / 4000) * reach
    scaled = np.stack([(x / reach) ** p for p in powers], 1)
    found = np.linalg.lstsq(scaled, function(x), rcond=None)[0]
    return [float(f / reach**p) for f, p in zip(found, powers)]


SIN = fit(np.sin, range(1, 16, 2))
COS = fit(np.cos, range(0, 17, 2))


def cos_sin(x):
    z = x * x
    sine = jnp.full_like(x, SIN[-1])
    for f in SIN[-2::-1]:
        sine = sine * z + f
    cosine = jnp.full_like(x, COS[-1])
    for f in COS[-2::-1]:
        cosine = cosine * z + f
    return cosine, sine * x


def bits_of(count):
    return count.bit_length() - 1


def pop(values, bits):
    total = values % 2
    for q in range(1, bits):
        total = total + (values // 2**q) % 2
    return total


def pop_array(values, bits):
    total = values & 1
    for q in range(1, bits):
        total = total + ((values >> q) & 1)
    return total


def mix_list(xs, turns):
    for q, (c, s) in enumerate(turns):
        step = 1 << q
        ys = list(xs)
        for i in range(len(xs)):
            if not i & step:
                u, v = xs[i], xs[i + step]
                ys[i] = c * u - s * v
                ys[i + step] = s * u + c * v
        xs = ys
    return xs


def mix_scaled(xs, tangents):
    for q, t in enumerate(tangents):
        step = 1 << q
        ys = list(xs)
        for i in range(len(xs)):
            if not i & step:
                u, v = xs[i], xs[i + step]
                ys[i] = u - t * v
                ys[i + step] = v + t * u
        xs = ys
    return xs


def rotation(count, c, s, transposed, mixed):
    i = lax.broadcasted_iota(jnp.int32, (count, count), 0)
    j = lax.broadcasted_iota(jnp.int32, (count, count), 1)
    if transposed:
        i, j = j, i
    c, s = c[:1, :count], s[:1, :count]
    table = jnp.where((i >> mixed) == (j >> mixed), 1.0, 0.0)
    for q in range(mixed):
        a, b = (i >> q) & 1, (j >> q) & 1
        table = table * jnp.where(a == b, c, jnp.where(a == 1, s, -s))
    return table


def split(x):
    hi = x.astype(BF16)
    return hi, (x - hi.astype(F32)).astype(BF16)


def kernel(nh, nl, parts, wave_hbm, level_hbm, diag_hbm, turn_hbm, home, tangent,
           diag, turn, wave, level, relay, abuf, recv, lev, back, lane_t, row_t,
           in_sem, reply, ready, relay_send, relay_recv, lev_send, lev_recv, to_send, to_recv, ret_send, ret_recv):
    n = nh * nl
    rp, lanes = level.shape[-2:]
    blocks, rows = wave.shape[1:3]
    cut = n // blocks
    rq = rp // parts
    h, l = lax.axis_index("high"), lax.axis_index("low")
    me = h * nl + l

    quad = nl // 4
    half = nl // 2

    zi, yi = l // quad, l % quad
    side = zi // 2
    partner = h * nl + (l ^ (3 * quad))
    edges = [(1 << i, 0, (h >> i) & 1) for i in range(bits_of(nh))]
    edges += [(0, 1 << i, (l >> i) & 1) for i in range(bits_of(quad))]
    edges += [(0, quad, zi % 2)]

    def call(body, dh, dl):
        body(dh * nl + dl, (dh, dl))

    def far_line(j):
        return jnp.where(zi < 2, 3 - j, j) * quad

    def far(body):
        def step(k, carry):
            t = k // nh
            call(body, h ^ (nh - 1 - k % nh), far_line(t // quad) + (yi ^ (quad - 1 - t % quad)))
            return carry
        lax.fori_loop(0, n // 2, step, 0)

    def near(body):
        def step(k, carry):
            call(body, h ^ (nh - 1 - k % nh), l ^ (half - 1 - k // nh))
            return carry
        lax.fori_loop(0, n // 2 - 1, step, 0)

    def others(body):
        near(body)
        far(body)

    barrier = pltpu.get_barrier_semaphore()

    def greet(sem):
        return lambda d, at: pl.semaphore_signal(sem, inc=1, device_id=at, device_id_type=MESH)

    def wait_reply(i):
        @pl.when(edges[i][2] == 0)
        def _():
            pl.semaphore_wait(reply.at[i], 1)

    call(greet(barrier), h, l ^ (3 * quad))
    for dh, dl, upper in edges:
        @pl.when(upper + side == 0)
        def _():
            call(greet(barrier), h ^ dh, l ^ dl)

    def level_in(which, i):
        return pltpu.make_async_copy(level_hbm.at[:, which], level.at[:, which], in_sem.at[i])

    wave_in = pltpu.make_async_copy(wave_hbm, wave, in_sem.at[1])
    diag_in = pltpu.make_async_copy(diag_hbm, diag, in_sem.at[2])
    turn_in = pltpu.make_async_copy(turn_hbm, turn, in_sem.at[3])
    pl.semaphore_wait(barrier, (1 - side) * sum(upper for _, _, upper in edges) + 1)

    relay_copy = pltpu.make_async_remote_copy(
        src_ref=level_hbm.at[:, 1 - side], dst_ref=relay, send_sem=relay_send, recv_sem=relay_recv,
        device_id=(h, l ^ (3 * quad)), device_id_type=MESH)
    relay_copy.start()
    level_in(1 - side, 0).start()
    level_in(side, 4).start()
    turn_in.start()
    diag_in.start()
    wave_in.start()

    @pl.when(side == 0)
    def _():
        for i, (dh, dl, upper) in enumerate(edges):
            @pl.when(upper == 1)
            def _():
                call(greet(reply.at[i]), h ^ dh, l ^ dl)
        for i in range(len(edges)):
            wait_reply(i)
        for i, (dh, dl, _) in enumerate(edges):
            call(greet(ready.at[i]), h ^ dh, l ^ dl)
            pl.semaphore_wait(ready.at[i], 1)
        call(greet(ready.at[len(edges)]), h, l ^ (3 * quad))

    @pl.when(side == 1)
    def _():
        pl.semaphore_wait(ready.at[len(edges)], 1)

    level_in(side, 4).wait()
    level_in(1 - side, 0).wait()

    def level_copy(d, at):
        return pltpu.make_async_remote_copy(
            src_ref=level.at[at[0], side, at[1] % half], dst_ref=lev.at[me],
            send_sem=lev_send, recv_sem=lev_recv,
            device_id=at, device_id_type=MESH)

    def pass_copy(d, at):
        return pltpu.make_async_remote_copy(
            src_ref=relay.at[at[0], at[1] % half], dst_ref=lev.at[partner],
            send_sem=lev_send, recv_sem=lev_recv,
            device_id=at, device_id_type=MESH)

    def to_copy(q):
        return lambda d, at: pltpu.make_async_remote_copy(
            src_ref=abuf.at[d, q], dst_ref=recv.at[me, q], send_sem=to_send.at[q],
            recv_sem=to_recv.at[q], device_id=at, device_id_type=MESH)

    def ret_copy(q):
        return lambda d, at: pltpu.make_async_remote_copy(
            src_ref=back.at[d, q], dst_ref=home.at[me, q],
            send_sem=ret_send.at[q], recv_sem=ret_recv.at[q],
            device_id=at, device_id_type=MESH)

    def wait_all(blocks_of, sem, count=n - 1):
        most = blocks_of(pl.ds(0, count))
        pltpu.make_async_copy(most, most, sem).wait()

    def start(copy):
        return lambda d, at: copy(d, at).start()

    near(start(level_copy))

    turn_in.wait()
    diag_in.wait()

    turns = []
    for layer in range(2):
        turns.append([cos_sin(jnp.full((8, lanes), turn[layer, g], F32)) for g in range(4)])
        c, s = turns[layer][0]
        hi, lo = split(rotation(lanes, c, s, True, bits_of(lanes)))
        lane_t[layer] = jnp.concatenate(
            [jnp.concatenate([hi, lo], 1), jnp.concatenate([hi, jnp.zeros_like(hi)], 1)], 0)
        c, s = turns[layer][1]
        hi, lo = split(rotation(rows, c, s, False, bits_of(rows if layer == 0 else rq)))
        row_t[layer] = jnp.concatenate(
            [jnp.concatenate([hi, hi], 1), jnp.concatenate([lo, jnp.zeros_like(hi)], 1)], 0)

    ones = pop_array(lax.broadcasted_iota(jnp.int32, (rows, lanes), 0), bits_of(rows)) + pop_array(
        lax.broadcasted_iota(jnp.int32, (rows, lanes), 1), bits_of(lanes))
    ones_dev = pop(me, bits_of(n))

    def mix_lanes(x, layer):
        hi, lo = split(x)
        z = jnp.dot(jnp.concatenate([hi, lo], 1), lane_t[layer], preferred_element_type=F32)
        return z[:, :lanes] + z[:, lanes:]

    def mix_rows(x, y, layer):
        hi, lo = split(jnp.concatenate([x, y], 1))
        z = jnp.dot(row_t[layer], jnp.concatenate([hi, lo], 0), preferred_element_type=F32)
        z = z[:rows] + z[rows:]
        return z[:, :lanes], z[:, lanes:]

    def mix_blocks(buf, middle_at, start, count, layer):
        pair = [turns[layer][2]] * bits_of(blocks)
        per = count // 8

        def body(t, carry):
            p, at = t // per, pl.ds(pl.multiple_of(start + (t % per) * 8, 8), 8)
            xs = mix_list([buf[b * cut + p, middle_at, at] for b in range(blocks)], pair)
            for b in range(blocks):
                buf[b * cut + p, middle_at, at] = xs[b]
            return carry
        lax.fori_loop(0, cut * per, body, 0)

    def quarter(count):
        k = (ones + count) & 3
        return (k & 1) == 1, jnp.where(k >= 2, -1.0, 1.0)

    wave_in.wait()
    lev[me] = level[h, side, l % half]

    def first(b, carry):
        slots = [b * cut + p for p in range(cut)]
        e = jnp.concatenate([level[d // nl, d % nl // half, d % half] for d in slots], 0)
        c, s = cos_sin(e * diag[pl.ds(0, 1), :])
        odd, sign = quarter(ones_dev + pop(b, bits_of(blocks)))
        cc = jnp.where(odd, s, c) * sign
        ss = jnp.where(odd, -c, s) * sign
        re, im = wave[0, b], wave[1, b]
        z = mix_lanes(jnp.concatenate([re * cc + im * ss, im * cc - re * ss], 0), 0)
        re, im = mix_rows(z[:rows], z[rows:], 0)
        for p in range(cut):
            for q in range(parts):
                at = p * rp + q * rq
                abuf[b * cut + p, q, :rq] = re[at:at + rq]
                abuf[b * cut + p, q, rq:] = im[at:at + rq]
        return carry
    lax.fori_loop(0, blocks, first, 0)
    for q in range(parts):
        mix_blocks(abuf, q, 0, 2 * rq, 0)
        others(start(to_copy(q)))
        recv[me, q] = abuf[me, q]
        if q == 0:
            relay_copy.wait_recv()
            near(start(pass_copy))
            lev[partner] = relay[h, l % half]

    def dev_turns(layer):
        return [turns[layer][3]] * bits_of(nl) + [turns[layer][2]] * bits_of(nh)

    def middle(q):
        def body(j, carry):
            at = pl.ds(pl.multiple_of(j * 8, 8), 8)
            at_im = pl.ds(pl.multiple_of(rq + j * 8, 8), 8)
            at_part = pl.ds(pl.multiple_of(q * rq + j * 8, 8), 8)
            xs = mix_list([recv[d, q, at] for d in range(n)], dev_turns(0))
            for d in range(n):
                recv[d, q, at] = xs[d]
            ys = mix_list([recv[d, q, at_im] for d in range(n)], dev_turns(0))
            angle = diag[pl.ds(1, 1), :]
            for d in range(n):
                c, s = cos_sin(lev[d, at_part] * angle)
                x, y = recv[d, q, at], ys[d]
                recv[d, q, at] = x * c + y * s
                ys[d] = y * c - x * s
            ys = mix_list(ys, dev_turns(1))
            for d in range(n):
                back[d, q, 1, at] = ys[d]
            xs = mix_list([recv[d, q, at] for d in range(n)], dev_turns(1))
            for d in range(n):
                back[d, q, 0, at] = xs[d]
            return carry
        lax.fori_loop(0, rq // 8, body, 0)

    tangents = [turns[1][g][1] / turns[1][g][0] for g in (1, 2)]
    own_tangents = [tangents[0]] * bits_of(cut) + [tangents[1]] * bits_of(blocks)
    tangent[0], tangent[1] = tangents
    scale = jnp.ones((1, lanes), F32)
    for g, count in ((1, bits_of(cut * parts)), (2, bits_of(blocks))):
        for _ in range(count):
            scale = scale * turns[1][g][0][:1]

    group = rows // rq

    def finish(q):
        def body(i, carry):
            ds = pl.ds(i * group, group)
            z = [back[ds, q, part].reshape(rows, lanes) for part in range(2)]
            z = mix_lanes(jnp.concatenate(z, 0), 1)
            re, im = mix_rows(z[:rows], z[rows:], 1)
            odd, sign = quarter(pop(i, bits_of(n // group)))
            sign = sign * scale
            back[ds, q, 0] = (jnp.where(odd, im, re) * sign).reshape(group, rq, lanes)
            back[ds, q, 1] = (jnp.where(odd, -re, im) * sign).reshape(group, rq, lanes)
            return carry
        lax.fori_loop(0, n // group, body, 0, unroll=2)

    wait_all(lambda d: lev.at[d], lev_recv, n - 2)
    for q in range(parts):
        wait_all(lambda d: recv.at[d, q], to_recv.at[q])
        middle(q)
        finish(q)
        others(start(ret_copy(q)))
    home[me] = back[me]

    relay_copy.wait_send()
    wait_all(lambda d: lev.at[d], lev_send, n - 2)
    for q in range(parts):
        wait_all(lambda d: abuf.at[d, q], to_send.at[q])

    def settle(q):
        def body(t, carry):
            at = pl.ds(pl.multiple_of(t * 8, 8), 8)
            for part in range(2):
                xs = mix_scaled([home[d, q, part, at] for d in range(n)], own_tangents)
                for d in range(n):
                    home[d, q, part, at] = xs[d]
            return carry
        lax.fori_loop(0, rq // 8, body, 0)

    for q in range(parts):
        wait_all(lambda d: home.at[d, q], ret_recv.at[q])
        if q < parts - 1:
            settle(q)
    for q in range(parts):
        wait_all(lambda d: back.at[d, q], ret_send.at[q])


def place(d, r, part):
    k = (d.bit_count() + r.bit_count() - part) % 4
    return k % 2, k in (1, 2)


def close(home, tangent, out_hbm, out, sem):
    n, parts, _, rq, lanes = home.shape
    blocks = out.shape[1]
    cut = n // blocks
    own_tangents = [tangent[0]] * bits_of(cut) + [tangent[1]] * bits_of(blocks)

    def out_copy(t):
        at = pl.ds(pl.multiple_of(t * 8, 8), 8)
        return pltpu.make_async_copy(
            out.at[:, :, :, :, at], out_hbm.at[:, :, :, :, at], sem.at[t])

    def body(t, carry):
        at = pl.ds(pl.multiple_of(t * 8, 8), 8)
        for part in range(2):
            xs = mix_scaled([home[d, parts - 1, part, at] for d in range(n)], own_tangents)
            for d in range(n):
                b, p = d // cut, d % cut
                ys = [home[d, r, part, at] for r in range(parts - 1)] + [xs[d]]
                ys = mix_scaled(ys, [tangent[0]] * bits_of(parts))
                for r in range(parts):
                    index, minus = place(d, r, part)
                    out[index, b, p, r, at] = -ys[r] if minus else ys[r]
        out_copy(t).start()
        return carry
    lax.fori_loop(0, rq // 8, body, 0)
    for t in range(rq // 8):
        out_copy(t).wait()


def solution(mesh):
    nh, nl = mesh.shape["high"], mesh.shape["low"]
    n = nh * nl

    def on_device(wave, level, diag, turn):
        blocks, rows, lanes = level.shape
        rp = rows // (n // blocks)
        level = level.reshape(nh, 2, nl // 2, rp, lanes)
        parts = 2 if rp % 16 == 0 else 1
        hbm = pl.BlockSpec(memory_space=pltpu.HBM)
        vmem = pl.BlockSpec(memory_space=pltpu.VMEM)
        dma = pltpu.SemaphoreType.DMA
        home, tangent = pl.pallas_call(
            functools.partial(kernel, nh, nl, parts),
            out_shape=(pltpu.VMEM((n, parts, 2, rp // parts, lanes), F32), pltpu.VMEM((2, 8, lanes), F32)),
            in_specs=[hbm] * 4,
            out_specs=(vmem, vmem),
            scratch_shapes=[
                pltpu.VMEM(diag.shape, F32),
                pltpu.SMEM(turn.shape, F32),
                pltpu.VMEM(wave.shape, F32),
                pltpu.VMEM(level.shape, F32),
                pltpu.VMEM((nh, nl // 2, rp, lanes), F32),
                pltpu.VMEM((n, parts, 2 * rp // parts, lanes), F32),
                pltpu.VMEM((n, parts, 2 * rp // parts, lanes), F32),
                pltpu.VMEM((n, rp, lanes), F32),
                pltpu.VMEM((n, parts, 2, rp // parts, lanes), F32),
                pltpu.VMEM((2, 2 * lanes, 2 * lanes), BF16),
                pltpu.VMEM((2, 2 * rows, 2 * rows), BF16),
                dma((5,)), *[pltpu.SemaphoreType.REGULAR((bits_of(n),))] * 2, dma, dma, dma, dma, dma((parts,)), dma((parts,)),
                dma((parts,)), dma((parts,)),
            ],
            compiler_params=pltpu.CompilerParams(
                collective_id=0, has_side_effects=True, vmem_limit_bytes=20 * 2**20),
        )(*[pltpu.with_memory_space_constraint(x, pltpu.HBM) for x in (wave, level, diag, turn)])
        split_shape = (2, blocks, n // blocks, parts, rp // parts, lanes)
        out = pl.pallas_call(
            close,
            out_shape=jax.ShapeDtypeStruct(split_shape, F32),
            in_specs=[vmem, vmem],
            out_specs=hbm,
            scratch_shapes=[pltpu.VMEM(split_shape, F32), dma((rp // parts // 8,))],
            compiler_params=pltpu.CompilerParams(vmem_limit_bytes=8 * 2**20),
        )(home, tangent)
        return out.reshape(wave.shape)

    in_specs = (P(None, ("high", "low"), None, None), P(("high", "low"), None, None), P(), P())
    return jax.shard_map(
        on_device, mesh=mesh, in_specs=in_specs,
        out_specs=P(None, ("high", "low"), None, None), check_vma=False)
```

```python
import functools

import jax
import jax.numpy as jnp
import numpy as np
from jax import lax
from jax.experimental import pallas as pl
from jax.experimental.pallas import tpu as pltpu
from jax.sharding import PartitionSpec as P

MESH = pl.DeviceIdType.MESH
F32 = jnp.float32
BF16 = jnp.bfloat16


def fit(function, powers, reach=3.2):
    x = np.cos(np.pi * (np.arange(4000) + 0.5) / 4000) * reach
    scaled = np.stack([(x / reach) ** p for p in powers], 1)
    found = np.linalg.lstsq(scaled, function(x), rcond=None)[0]
    return [float(f / reach**p) for f, p in zip(found, powers)]


SIN = fit(np.sin, range(1, 16, 2))
COS = fit(np.cos, range(0, 17, 2))


def cos_sin(x):
    z = x * x
    sine = jnp.full_like(x, SIN[-1])
    for f in SIN[-2::-1]:
        sine = sine * z + f
    cosine = jnp.full_like(x, COS[-1])
    for f in COS[-2::-1]:
        cosine = cosine * z + f
    return cosine, sine * x


def bits_of(count):
    return count.bit_length() - 1


def pop(values, bits):
    total = values % 2
    for q in range(1, bits):
        total = total + (values // 2**q) % 2
    return total


def pop_array(values, bits):
    total = values & 1
    for q in range(1, bits):
        total = total + ((values >> q) & 1)
    return total


def mix_list(xs, turns):
    for q, (c, s) in enumerate(turns):
        step = 1 << q
        ys = list(xs)
        for i in range(len(xs)):
            if not i & step:
                u, v = xs[i], xs[i + step]
                ys[i] = c * u - s * v
                ys[i + step] = s * u + c * v
        xs = ys
    return xs


def mix_scaled(xs, tangents):
    for q, t in enumerate(tangents):
        step = 1 << q
        ys = list(xs)
        for i in range(len(xs)):
            if not i & step:
                u, v = xs[i], xs[i + step]
                ys[i] = u - t * v
                ys[i + step] = v + t * u
        xs = ys
    return xs


def rotation(count, c, s, transposed, mixed):
    i = lax.broadcasted_iota(jnp.int32, (count, count), 0)
    j = lax.broadcasted_iota(jnp.int32, (count, count), 1)
    if transposed:
        i, j = j, i
    c, s = c[:1, :count], s[:1, :count]
    table = jnp.where((i >> mixed) == (j >> mixed), 1.0, 0.0)
    for q in range(mixed):
        a, b = (i >> q) & 1, (j >> q) & 1
        table = table * jnp.where(a == b, c, jnp.where(a == 1, s, -s))
    return table


def split(x):
    hi = x.astype(BF16)
    return hi, (x - hi.astype(F32)).astype(BF16)


def kernel(nh, nl, parts, wave_hbm, level_hbm, diag_hbm, turn_hbm, home, tangent,
           diag, turn, wave, level, relay, abuf, recv, lev, back, lane_t, row_t,
           in_sem, reply, ready, relay_send, relay_recv, lev_send, lev_recv, to_send, to_recv, ret_send, ret_recv):
    n = nh * nl
    rp, lanes = level.shape[-2:]
    blocks, rows = wave.shape[1:3]
    cut = n // blocks
    rq = rp // parts
    h, l = lax.axis_index("high"), lax.axis_index("low")
    me = h * nl + l

    quad = nl // 4
    half = nl // 2

    zi, yi = l // quad, l % quad
    side = zi // 2
    partner = h * nl + (l ^ (3 * quad))
    edges = [(1 << i, 0, (h >> i) & 1) for i in range(bits_of(nh))]
    edges += [(0, 1 << i, (l >> i) & 1) for i in range(bits_of(quad))]
    edges += [(0, quad, zi % 2)]

    def call(body, dh, dl):
        body(dh * nl + dl, (dh, dl))

    def far_line(j):
        return jnp.where(zi < 2, 3 - j, j) * quad

    def far(body):
        def step(k, carry):
            t = k // nh
            call(body, h ^ (nh - 1 - k % nh), far_line(t // quad) + (yi ^ (quad - 1 - t % quad)))
            return carry
        lax.fori_loop(0, n // 2, step, 0)

    def near(body):
        def step(k, carry):
            call(body, h ^ (nh - 1 - k % nh), l ^ (half - 1 - k // nh))
            return carry
        lax.fori_loop(0, n // 2 - 1, step, 0)

    def others(body):
        far(body)
        near(body)

    barrier = pltpu.get_barrier_semaphore()

    def greet(sem):
        return lambda d, at: pl.semaphore_signal(sem, inc=1, device_id=at, device_id_type=MESH)

    def wait_reply(i):
        @pl.when(edges[i][2] == 0)
        def _():
            pl.semaphore_wait(reply.at[i], 1)

    call(greet(barrier), h, l ^ (3 * quad))
    for dh, dl, upper in edges:
        @pl.when(upper + side == 0)
        def _():
            call(greet(barrier), h ^ dh, l ^ dl)

    def level_in(which, i):
        return pltpu.make_async_copy(level_hbm.at[:, which], level.at[:, which], in_sem.at[i])

    wave_in = pltpu.make_async_copy(wave_hbm, wave, in_sem.at[1])
    diag_in = pltpu.make_async_copy(diag_hbm, diag, in_sem.at[2])
    turn_in = pltpu.make_async_copy(turn_hbm, turn, in_sem.at[3])
    pl.semaphore_wait(barrier, (1 - side) * sum(upper for _, _, upper in edges) + 1)

    relay_copy = pltpu.make_async_remote_copy(
        src_ref=level_hbm.at[:, 1 - side], dst_ref=relay, send_sem=relay_send, recv_sem=relay_recv,
        device_id=(h, l ^ (3 * quad)), device_id_type=MESH)
    relay_copy.start()
    level_in(1 - side, 0).start()
    level_in(side, 4).start()
    turn_in.start()
    diag_in.start()
    wave_in.start()

    @pl.when(side == 0)
    def _():
        for i, (dh, dl, upper) in enumerate(edges):
            @pl.when(upper == 1)
            def _():
                call(greet(reply.at[i]), h ^ dh, l ^ dl)
        for i in range(len(edges)):
            wait_reply(i)
        for i, (dh, dl, _) in enumerate(edges):
            call(greet(ready.at[i]), h ^ dh, l ^ dl)
            pl.semaphore_wait(ready.at[i], 1)
        call(greet(ready.at[len(edges)]), h, l ^ (3 * quad))

    @pl.when(side == 1)
    def _():
        pl.semaphore_wait(ready.at[len(edges)], 1)

    level_in(side, 4).wait()
    level_in(1 - side, 0).wait()

    def level_copy(d, at):
        return pltpu.make_async_remote_copy(
            src_ref=level.at[at[0], side, at[1] % half], dst_ref=lev.at[me],
            send_sem=lev_send, recv_sem=lev_recv,
            device_id=at, device_id_type=MESH)

    def pass_copy(d, at):
        return pltpu.make_async_remote_copy(
            src_ref=relay.at[at[0], at[1] % half], dst_ref=lev.at[partner],
            send_sem=lev_send, recv_sem=lev_recv,
            device_id=at, device_id_type=MESH)

    def to_copy(q):
        return lambda d, at: pltpu.make_async_remote_copy(
            src_ref=abuf.at[d, q], dst_ref=recv.at[me, q], send_sem=to_send.at[q],
            recv_sem=to_recv.at[q], device_id=at, device_id_type=MESH)

    def ret_copy(q):
        return lambda d, at: pltpu.make_async_remote_copy(
            src_ref=back.at[d, q], dst_ref=home.at[me, q],
            send_sem=ret_send.at[q], recv_sem=ret_recv.at[q],
            device_id=at, device_id_type=MESH)

    def wait_all(blocks_of, sem, count=n - 1):
        most = blocks_of(pl.ds(0, count))
        pltpu.make_async_copy(most, most, sem).wait()

    def start(copy):
        return lambda d, at: copy(d, at).start()

    near(start(level_copy))

    turn_in.wait()
    diag_in.wait()

    turns = []
    for layer in range(2):
        turns.append([cos_sin(jnp.full((8, lanes), turn[layer, g], F32)) for g in range(4)])
        c, s = turns[layer][0]
        hi, lo = split(rotation(lanes, c, s, True, bits_of(lanes)))
        lane_t[layer] = jnp.concatenate(
            [jnp.concatenate([hi, lo], 1), jnp.concatenate([hi, jnp.zeros_like(hi)], 1)], 0)
        c, s = turns[layer][1]
        hi, lo = split(rotation(rows, c, s, False, bits_of(rows if layer == 0 else rq)))
        row_t[layer] = jnp.concatenate(
            [jnp.concatenate([hi, hi], 1), jnp.concatenate([lo, jnp.zeros_like(hi)], 1)], 0)

    ones = pop_array(lax.broadcasted_iota(jnp.int32, (rows, lanes), 0), bits_of(rows)) + pop_array(
        lax.broadcasted_iota(jnp.int32, (rows, lanes), 1), bits_of(lanes))
    ones_dev = pop(me, bits_of(n))

    def mix_lanes(x, layer):
        hi, lo = split(x)
        z = jnp.dot(jnp.concatenate([hi, lo], 1), lane_t[layer], preferred_element_type=F32)
        return z[:, :lanes] + z[:, lanes:]

    def mix_rows(x, y, layer):
        hi, lo = split(jnp.concatenate([x, y], 1))
        z = jnp.dot(row_t[layer], jnp.concatenate([hi, lo], 0), preferred_element_type=F32)
        z = z[:rows] + z[rows:]
        return z[:, :lanes], z[:, lanes:]

    def mix_blocks(buf, middle_at, start, count, layer):
        pair = [turns[layer][2]] * bits_of(blocks)
        per = count // 8

        def body(t, carry):
            p, at = t // per, pl.ds(pl.multiple_of(start + (t % per) * 8, 8), 8)
            xs = mix_list([buf[b * cut + p, middle_at, at] for b in range(blocks)], pair)
            for b in range(blocks):
                buf[b * cut + p, middle_at, at] = xs[b]
            return carry
        lax.fori_loop(0, cut * per, body, 0)

    def quarter(count):
        k = (ones + count) & 3
        return (k & 1) == 1, jnp.where(k >= 2, -1.0, 1.0)

    wave_in.wait()
    lev[me] = level[h, side, l % half]

    def first(b, carry):
        slots = [b * cut + p for p in range(cut)]
        e = jnp.concatenate([level[d // nl, d % nl // half, d % half] for d in slots], 0)
        c, s = cos_sin(e * diag[pl.ds(0, 1), :])
        odd, sign = quarter(ones_dev + pop(b, bits_of(blocks)))
        cc = jnp.where(odd, s, c) * sign
        ss = jnp.where(odd, -c, s) * sign
        re, im = wave[0, b], wave[1, b]
        z = mix_lanes(jnp.concatenate([re * cc + im * ss, im * cc - re * ss], 0), 0)
        re, im = mix_rows(z[:rows], z[rows:], 0)
        for p in range(cut):
            for q in range(parts):
                at = p * rp + q * rq
                abuf[b * cut + p, q, :rq] = re[at:at + rq]
                abuf[b * cut + p, q, rq:] = im[at:at + rq]
        return carry
    lax.fori_loop(0, blocks, first, 0)
    for q in range(parts):
        mix_blocks(abuf, q, 0, 2 * rq, 0)
        others(start(to_copy(q)))
        recv[me, q] = abuf[me, q]
        if q == 0:
            relay_copy.wait_recv()
            near(start(pass_copy))
            lev[partner] = relay[h, l % half]

    def dev_turns(layer):
        return [turns[layer][3]] * bits_of(nl) + [turns[layer][2]] * bits_of(nh)

    def middle(q):
        def body(j, carry):
            at = pl.ds(pl.multiple_of(j * 8, 8), 8)
            at_im = pl.ds(pl.multiple_of(rq + j * 8, 8), 8)
            at_part = pl.ds(pl.multiple_of(q * rq + j * 8, 8), 8)
            xs = mix_list([recv[d, q, at] for d in range(n)], dev_turns(0))
            for d in range(n):
                recv[d, q, at] = xs[d]
            ys = mix_list([recv[d, q, at_im] for d in range(n)], dev_turns(0))
            angle = diag[pl.ds(1, 1), :]
            for d in range(n):
                c, s = cos_sin(lev[d, at_part] * angle)
                x, y = recv[d, q, at], ys[d]
                recv[d, q, at] = x * c + y * s
                ys[d] = y * c - x * s
            ys = mix_list(ys, dev_turns(1))
            for d in range(n):
                back[d, q, 1, at] = ys[d]
            xs = mix_list([recv[d, q, at] for d in range(n)], dev_turns(1))
            for d in range(n):
                back[d, q, 0, at] = xs[d]
            return carry
        lax.fori_loop(0, rq // 8, body, 0)

    tangents = [turns[1][g][1] / turns[1][g][0] for g in (1, 2)]
    own_tangents = [tangents[0]] * bits_of(cut) + [tangents[1]] * bits_of(blocks)
    tangent[0], tangent[1] = tangents
    scale = jnp.ones((1, lanes), F32)
    for g, count in ((1, bits_of(cut * parts)), (2, bits_of(blocks))):
        for _ in range(count):
            scale = scale * turns[1][g][0][:1]

    group = rows // rq

    def finish(q):
        def body(i, carry):
            ds = pl.ds(i * group, group)
            z = [back[ds, q, part].reshape(rows, lanes) for part in range(2)]
            z = mix_lanes(jnp.concatenate(z, 0), 1)
            re, im = mix_rows(z[:rows], z[rows:], 1)
            odd, sign = quarter(pop(i, bits_of(n // group)))
            sign = sign * scale
            back[ds, q, 0] = (jnp.where(odd, im, re) * sign).reshape(group, rq, lanes)
            back[ds, q, 1] = (jnp.where(odd, -re, im) * sign).reshape(group, rq, lanes)
            return carry
        lax.fori_loop(0, n // group, body, 0, unroll=2)

    wait_all(lambda d: lev.at[d], lev_recv, n - 2)
    for q in range(parts):
        wait_all(lambda d: recv.at[d, q], to_recv.at[q])
        middle(q)
        finish(q)
        others(start(ret_copy(q)))
    home[me] = back[me]

    relay_copy.wait_send()
    wait_all(lambda d: lev.at[d], lev_send, n - 2)
    for q in range(parts):
        wait_all(lambda d: abuf.at[d, q], to_send.at[q])

    def settle(q):
        def body(t, carry):
            at = pl.ds(pl.multiple_of(t * 8, 8), 8)
            for part in range(2):
                xs = mix_scaled([home[d, q, part, at] for d in range(n)], own_tangents)
                for d in range(n):
                    home[d, q, part, at] = xs[d]
            return carry
        lax.fori_loop(0, rq // 8, body, 0)

    for q in range(parts):
        wait_all(lambda d: home.at[d, q], ret_recv.at[q])
        if q < parts - 1:
            settle(q)
    for q in range(parts):
        wait_all(lambda d: back.at[d, q], ret_send.at[q])


def place(d, r, part):
    k = (d.bit_count() + r.bit_count() - part) % 4
    return k % 2, k in (1, 2)


def close(home, tangent, out_hbm, out, sem):
    n, parts, _, rq, lanes = home.shape
    blocks = out.shape[1]
    cut = n // blocks
    own_tangents = [tangent[0]] * bits_of(cut) + [tangent[1]] * bits_of(blocks)

    def out_copy(t):
        at = pl.ds(pl.multiple_of(t * 8, 8), 8)
        return pltpu.make_async_copy(
            out.at[:, :, :, :, at], out_hbm.at[:, :, :, :, at], sem.at[t])

    def body(t, carry):
        at = pl.ds(pl.multiple_of(t * 8, 8), 8)
        for part in range(2):
            xs = mix_scaled([home[d, parts - 1, part, at] for d in range(n)], own_tangents)
            for d in range(n):
                b, p = d // cut, d % cut
                ys = [home[d, r, part, at] for r in range(parts - 1)] + [xs[d]]
                ys = mix_scaled(ys, [tangent[0]] * bits_of(parts))
                for r in range(parts):
                    index, minus = place(d, r, part)
                    out[index, b, p, r, at] = -ys[r] if minus else ys[r]
        out_copy(t).start()
        return carry
    lax.fori_loop(0, rq // 8, body, 0)
    for t in range(rq // 8):
        out_copy(t).wait()


def solution(mesh):
    nh, nl = mesh.shape["high"], mesh.shape["low"]
    n = nh * nl

    def on_device(wave, level, diag, turn):
        blocks, rows, lanes = level.shape
        rp = rows // (n // blocks)
        level = level.reshape(nh, 2, nl // 2, rp, lanes)
        parts = 2 if rp % 16 == 0 else 1
        hbm = pl.BlockSpec(memory_space=pltpu.HBM)
        vmem = pl.BlockSpec(memory_space=pltpu.VMEM)
        dma = pltpu.SemaphoreType.DMA
        home, tangent = pl.pallas_call(
            functools.partial(kernel, nh, nl, parts),
            out_shape=(pltpu.VMEM((n, parts, 2, rp // parts, lanes), F32), pltpu.VMEM((2, 8, lanes), F32)),
            in_specs=[hbm] * 4,
            out_specs=(vmem, vmem),
            scratch_shapes=[
                pltpu.VMEM(diag.shape, F32),
                pltpu.SMEM(turn.shape, F32),
                pltpu.VMEM(wave.shape, F32),
                pltpu.VMEM(level.shape, F32),
                pltpu.VMEM((nh, nl // 2, rp, lanes), F32),
                pltpu.VMEM((n, parts, 2 * rp // parts, lanes), F32),
                pltpu.VMEM((n, parts, 2 * rp // parts, lanes), F32),
                pltpu.VMEM((n, rp, lanes), F32),
                pltpu.VMEM((n, parts, 2, rp // parts, lanes), F32),
                pltpu.VMEM((2, 2 * lanes, 2 * lanes), BF16),
                pltpu.VMEM((2, 2 * rows, 2 * rows), BF16),
                dma((5,)), *[pltpu.SemaphoreType.REGULAR((bits_of(n),))] * 2, dma, dma, dma, dma, dma((parts,)), dma((parts,)),
                dma((parts,)), dma((parts,)),
            ],
            compiler_params=pltpu.CompilerParams(
                collective_id=0, has_side_effects=True, vmem_limit_bytes=20 * 2**20),
        )(*[pltpu.with_memory_space_constraint(x, pltpu.HBM) for x in (wave, level, diag, turn)])
        split_shape = (2, blocks, n // blocks, parts, rp // parts, lanes)
        out = pl.pallas_call(
            close,
            out_shape=jax.ShapeDtypeStruct(split_shape, F32),
            in_specs=[vmem, vmem],
            out_specs=hbm,
            scratch_shapes=[pltpu.VMEM(split_shape, F32), dma((rp // parts // 8,))],
            compiler_params=pltpu.CompilerParams(vmem_limit_bytes=8 * 2**20),
        )(home, tangent)
        return out.reshape(wave.shape)

    in_specs = (P(None, ("high", "low"), None, None), P(("high", "low"), None, None), P(), P())
    return jax.shard_map(
        on_device, mesh=mesh, in_specs=in_specs,
        out_specs=P(None, ("high", "low"), None, None), check_vma=False)
```

```python
import functools

import jax
import jax.numpy as jnp
import numpy as np
from jax import lax
from jax.experimental import pallas as pl
from jax.experimental.pallas import tpu as pltpu
from jax.sharding import PartitionSpec as P

MESH = pl.DeviceIdType.MESH
F32 = jnp.float32
BF16 = jnp.bfloat16


def fit(function, powers, reach=3.2):
    x = np.cos(np.pi * (np.arange(4000) + 0.5) / 4000) * reach
    scaled = np.stack([(x / reach) ** p for p in powers], 1)
    found = np.linalg.lstsq(scaled, function(x), rcond=None)[0]
    return [float(f / reach**p) for f, p in zip(found, powers)]


SIN = fit(np.sin, range(1, 16, 2))
COS = fit(np.cos, range(0, 17, 2))


def cos_sin(x):
    z = x * x
    sine = jnp.full_like(x, SIN[-1])
    for f in SIN[-2::-1]:
        sine = sine * z + f
    cosine = jnp.full_like(x, COS[-1])
    for f in COS[-2::-1]:
        cosine = cosine * z + f
    return cosine, sine * x


def bits_of(count):
    return count.bit_length() - 1


def pop(values, bits):
    total = values % 2
    for q in range(1, bits):
        total = total + (values // 2**q) % 2
    return total


def pop_array(values, bits):
    total = values & 1
    for q in range(1, bits):
        total = total + ((values >> q) & 1)
    return total


def mix_list(xs, turns):
    for q, (c, s) in enumerate(turns):
        step = 1 << q
        ys = list(xs)
        for i in range(len(xs)):
            if not i & step:
                u, v = xs[i], xs[i + step]
                ys[i] = c * u - s * v
                ys[i + step] = s * u + c * v
        xs = ys
    return xs


def mix_scaled(xs, tangents):
    for q, t in enumerate(tangents):
        step = 1 << q
        ys = list(xs)
        for i in range(len(xs)):
            if not i & step:
                u, v = xs[i], xs[i + step]
                ys[i] = u - t * v
                ys[i + step] = v + t * u
        xs = ys
    return xs


def rotation(count, c, s, transposed, mixed):
    i = lax.broadcasted_iota(jnp.int32, (count, count), 0)
    j = lax.broadcasted_iota(jnp.int32, (count, count), 1)
    if transposed:
        i, j = j, i
    c, s = c[:1, :count], s[:1, :count]
    table = jnp.where((i >> mixed) == (j >> mixed), 1.0, 0.0)
    for q in range(mixed):
        a, b = (i >> q) & 1, (j >> q) & 1
        table = table * jnp.where(a == b, c, jnp.where(a == 1, s, -s))
    return table


def split(x):
    hi = x.astype(BF16)
    return hi, (x - hi.astype(F32)).astype(BF16)


def kernel(nh, nl, parts, wave_hbm, level_hbm, diag_hbm, turn_hbm, home, tangent,
           diag, turn, wave, level, relay, abuf, recv, lev, back, lane_t, row_t,
           in_sem, reply, ready, relay_send, relay_recv, lev_send, lev_recv, to_send, to_recv, ret_send, ret_recv):
    n = nh * nl
    rp, lanes = level.shape[-2:]
    blocks, rows = wave.shape[1:3]
    cut = n // blocks
    rq = rp // parts
    h, l = lax.axis_index("high"), lax.axis_index("low")
    me = h * nl + l

    quad = nl // 4
    half = nl // 2

    zi, yi = l // quad, l % quad
    side = zi // 2
    partner = h * nl + (l ^ (3 * quad))
    edges = [(1 << i, 0, (h >> i) & 1) for i in range(bits_of(nh))]
    edges += [(0, 1 << i, (l >> i) & 1) for i in range(bits_of(quad))]
    edges += [(0, quad, zi % 2)]

    def call(body, dh, dl):
        body(dh * nl + dl, (dh, dl))

    def far_line(j):
        return jnp.where(zi < 2, 3 - j, j) * quad

    def far(body):
        def step(k, carry):
            t = k // nh
            call(body, h ^ (nh - 1 - k % nh), far_line(t // quad) + (yi ^ (quad - 1 - t % quad)))
            return carry
        lax.fori_loop(0, n // 2, step, 0)

    def near(body):
        def step(k, carry):
            call(body, h ^ (nh - 1 - k % nh), l ^ (half - 1 - k // nh))
            return carry
        lax.fori_loop(0, n // 2 - 1, step, 0)

    def others(body):
        near(body)
        far(body)

    barrier = pltpu.get_barrier_semaphore()

    def greet(sem):
        return lambda d, at: pl.semaphore_signal(sem, inc=1, device_id=at, device_id_type=MESH)

    def wait_reply(i):
        @pl.when(edges[i][2] == 0)
        def _():
            pl.semaphore_wait(reply.at[i], 1)

    call(greet(barrier), h, l ^ (3 * quad))
    for dh, dl, upper in edges:
        @pl.when(upper + side == 0)
        def _():
            call(greet(barrier), h ^ dh, l ^ dl)

    def level_in(which, i):
        return pltpu.make_async_copy(level_hbm.at[:, which], level.at[:, which], in_sem.at[i])

    wave_in = pltpu.make_async_copy(wave_hbm, wave, in_sem.at[1])
    diag_in = pltpu.make_async_copy(diag_hbm, diag, in_sem.at[2])
    turn_in = pltpu.make_async_copy(turn_hbm, turn, in_sem.at[3])
    @pl.when(side == 0)
    def _():
        level_in(1 - side, 0).start()

    pl.semaphore_wait(barrier, (1 - side) * sum(upper for _, _, upper in edges) + 1)

    def relay_from(table):
        return pltpu.make_async_remote_copy(
            src_ref=table.at[:, 1 - side], dst_ref=relay, send_sem=relay_send, recv_sem=relay_recv,
            device_id=(h, l ^ (3 * quad)), device_id_type=MESH)

    relay_copy = relay_from(level_hbm)

    @pl.when(side == 0)
    def _():
        level_in(1 - side, 0).wait()
        relay_from(level).start()

    @pl.when(side == 1)
    def _():
        relay_copy.start()
        level_in(1 - side, 0).start()

    level_in(side, 4).start()
    turn_in.start()
    diag_in.start()
    wave_in.start()

    @pl.when(side == 0)
    def _():
        for i, (dh, dl, upper) in enumerate(edges):
            @pl.when(upper == 1)
            def _():
                call(greet(reply.at[i]), h ^ dh, l ^ dl)
        for i in range(len(edges)):
            wait_reply(i)
        for i, (dh, dl, _) in enumerate(edges):
            call(greet(ready.at[i]), h ^ dh, l ^ dl)
            pl.semaphore_wait(ready.at[i], 1)
        call(greet(ready.at[len(edges)]), h, l ^ (3 * quad))

    @pl.when(side == 1)
    def _():
        pl.semaphore_wait(ready.at[len(edges)], 1)

    level_in(side, 4).wait()

    @pl.when(side == 1)
    def _():
        level_in(1 - side, 0).wait()

    def level_copy(d, at):
        return pltpu.make_async_remote_copy(
            src_ref=level.at[at[0], side, at[1] % half], dst_ref=lev.at[me],
            send_sem=lev_send, recv_sem=lev_recv,
            device_id=at, device_id_type=MESH)

    def pass_copy(d, at):
        return pltpu.make_async_remote_copy(
            src_ref=relay.at[at[0], at[1] % half], dst_ref=lev.at[partner],
            send_sem=lev_send, recv_sem=lev_recv,
            device_id=at, device_id_type=MESH)

    def to_copy(q):
        return lambda d, at: pltpu.make_async_remote_copy(
            src_ref=abuf.at[d, q], dst_ref=recv.at[me, q], send_sem=to_send.at[q],
            recv_sem=to_recv.at[q], device_id=at, device_id_type=MESH)

    def ret_copy(q):
        return lambda d, at: pltpu.make_async_remote_copy(
            src_ref=back.at[d, q], dst_ref=home.at[me, q],
            send_sem=ret_send.at[q], recv_sem=ret_recv.at[q],
            device_id=at, device_id_type=MESH)

    def wait_all(blocks_of, sem, count=n - 1):
        most = blocks_of(pl.ds(0, count))
        pltpu.make_async_copy(most, most, sem).wait()

    def start(copy):
        return lambda d, at: copy(d, at).start()

    near(start(level_copy))

    turn_in.wait()
    diag_in.wait()

    turns = []
    for layer in range(2):
        turns.append([cos_sin(jnp.full((8, lanes), turn[layer, g], F32)) for g in range(4)])
        c, s = turns[layer][0]
        hi, lo = split(rotation(lanes, c, s, True, bits_of(lanes)))
        lane_t[layer] = jnp.concatenate(
            [jnp.concatenate([hi, lo], 1), jnp.concatenate([hi, jnp.zeros_like(hi)], 1)], 0)
        c, s = turns[layer][1]
        hi, lo = split(rotation(rows, c, s, False, bits_of(rows if layer == 0 else rq)))
        row_t[layer] = jnp.concatenate(
            [jnp.concatenate([hi, hi], 1), jnp.concatenate([lo, jnp.zeros_like(hi)], 1)], 0)

    ones = pop_array(lax.broadcasted_iota(jnp.int32, (rows, lanes), 0), bits_of(rows)) + pop_array(
        lax.broadcasted_iota(jnp.int32, (rows, lanes), 1), bits_of(lanes))
    ones_dev = pop(me, bits_of(n))

    def mix_lanes(x, layer):
        hi, lo = split(x)
        z = jnp.dot(jnp.concatenate([hi, lo], 1), lane_t[layer], preferred_element_type=F32)
        return z[:, :lanes] + z[:, lanes:]

    def mix_rows(x, y, layer):
        hi, lo = split(jnp.concatenate([x, y], 1))
        z = jnp.dot(row_t[layer], jnp.concatenate([hi, lo], 0), preferred_element_type=F32)
        z = z[:rows] + z[rows:]
        return z[:, :lanes], z[:, lanes:]

    def mix_blocks(buf, middle_at, start, count, layer):
        pair = [turns[layer][2]] * bits_of(blocks)
        per = count // 8

        def body(t, carry):
            p, at = t // per, pl.ds(pl.multiple_of(start + (t % per) * 8, 8), 8)
            xs = mix_list([buf[b * cut + p, middle_at, at] for b in range(blocks)], pair)
            for b in range(blocks):
                buf[b * cut + p, middle_at, at] = xs[b]
            return carry
        lax.fori_loop(0, cut * per, body, 0)

    def quarter(count):
        k = (ones + count) & 3
        return (k & 1) == 1, jnp.where(k >= 2, -1.0, 1.0)

    wave_in.wait()
    lev[me] = level[h, side, l % half]

    def first(b, carry):
        slots = [b * cut + p for p in range(cut)]
        e = jnp.concatenate([level[d // nl, d % nl // half, d % half] for d in slots], 0)
        c, s = cos_sin(e * diag[pl.ds(0, 1), :])
        odd, sign = quarter(ones_dev + pop(b, bits_of(blocks)))
        cc = jnp.where(odd, s, c) * sign
        ss = jnp.where(odd, -c, s) * sign
        re, im = wave[0, b], wave[1, b]
        z = mix_lanes(jnp.concatenate([re * cc + im * ss, im * cc - re * ss], 0), 0)
        re, im = mix_rows(z[:rows], z[rows:], 0)
        for p in range(cut):
            for q in range(parts):
                at = p * rp + q * rq
                abuf[b * cut + p, q, :rq] = re[at:at + rq]
                abuf[b * cut + p, q, rq:] = im[at:at + rq]
        return carry
    lax.fori_loop(0, blocks, first, 0)
    for q in range(parts):
        mix_blocks(abuf, q, 0, 2 * rq, 0)
        others(start(to_copy(q)))
        recv[me, q] = abuf[me, q]
        if q == 0:
            relay_copy.wait_recv()
            near(start(pass_copy))
            lev[partner] = relay[h, l % half]

    def dev_turns(layer):
        return [turns[layer][3]] * bits_of(nl) + [turns[layer][2]] * bits_of(nh)

    def middle(q):
        def body(j, carry):
            at = pl.ds(pl.multiple_of(j * 8, 8), 8)
            at_im = pl.ds(pl.multiple_of(rq + j * 8, 8), 8)
            at_part = pl.ds(pl.multiple_of(q * rq + j * 8, 8), 8)
            xs = mix_list([recv[d, q, at] for d in range(n)], dev_turns(0))
            for d in range(n):
                recv[d, q, at] = xs[d]
            ys = mix_list([recv[d, q, at_im] for d in range(n)], dev_turns(0))
            angle = diag[pl.ds(1, 1), :]
            for d in range(n):
                c, s = cos_sin(lev[d, at_part] * angle)
                x, y = recv[d, q, at], ys[d]
                recv[d, q, at] = x * c + y * s
                ys[d] = y * c - x * s
            ys = mix_list(ys, dev_turns(1))
            for d in range(n):
                back[d, q, 1, at] = ys[d]
            xs = mix_list([recv[d, q, at] for d in range(n)], dev_turns(1))
            for d in range(n):
                back[d, q, 0, at] = xs[d]
            return carry
        lax.fori_loop(0, rq // 8, body, 0)

    tangents = [turns[1][g][1] / turns[1][g][0] for g in (1, 2)]
    own_tangents = [tangents[0]] * bits_of(cut) + [tangents[1]] * bits_of(blocks)
    tangent[0], tangent[1] = tangents
    scale = jnp.ones((1, lanes), F32)
    for g, count in ((1, bits_of(cut * parts)), (2, bits_of(blocks))):
        for _ in range(count):
            scale = scale * turns[1][g][0][:1]

    group = rows // rq

    def finish(q):
        def body(i, carry):
            ds = pl.ds(i * group, group)
            z = [back[ds, q, part].reshape(rows, lanes) for part in range(2)]
            z = mix_lanes(jnp.concatenate(z, 0), 1)
            re, im = mix_rows(z[:rows], z[rows:], 1)
            odd, sign = quarter(pop(i, bits_of(n // group)))
            sign = sign * scale
            back[ds, q, 0] = (jnp.where(odd, im, re) * sign).reshape(group, rq, lanes)
            back[ds, q, 1] = (jnp.where(odd, -re, im) * sign).reshape(group, rq, lanes)
            return carry
        lax.fori_loop(0, n // group, body, 0, unroll=2)

    wait_all(lambda d: lev.at[d], lev_recv, n - 2)
    for q in range(parts):
        wait_all(lambda d: recv.at[d, q], to_recv.at[q])
        middle(q)
        finish(q)
        others(start(ret_copy(q)))
    home[me] = back[me]

    relay_copy.wait_send()
    wait_all(lambda d: lev.at[d], lev_send, n - 2)
    for q in range(parts):
        wait_all(lambda d: abuf.at[d, q], to_send.at[q])

    def settle(q):
        def body(t, carry):
            at = pl.ds(pl.multiple_of(t * 8, 8), 8)
            for part in range(2):
                xs = mix_scaled([home[d, q, part, at] for d in range(n)], own_tangents)
                for d in range(n):
                    home[d, q, part, at] = xs[d]
            return carry
        lax.fori_loop(0, rq // 8, body, 0)

    for q in range(parts):
        wait_all(lambda d: home.at[d, q], ret_recv.at[q])
        if q < parts - 1:
            settle(q)
    for q in range(parts):
        wait_all(lambda d: back.at[d, q], ret_send.at[q])


def place(d, r, part):
    k = (d.bit_count() + r.bit_count() - part) % 4
    return k % 2, k in (1, 2)


def close(home, tangent, out_hbm, out, sem):
    n, parts, _, rq, lanes = home.shape
    blocks = out.shape[1]
    cut = n // blocks
    own_tangents = [tangent[0]] * bits_of(cut) + [tangent[1]] * bits_of(blocks)

    def out_copy(t):
        at = pl.ds(pl.multiple_of(t * 8, 8), 8)
        return pltpu.make_async_copy(
            out.at[:, :, :, :, at], out_hbm.at[:, :, :, :, at], sem.at[t])

    def body(t, carry):
        at = pl.ds(pl.multiple_of(t * 8, 8), 8)
        for part in range(2):
            xs = mix_scaled([home[d, parts - 1, part, at] for d in range(n)], own_tangents)
            for d in range(n):
                b, p = d // cut, d % cut
                ys = [home[d, r, part, at] for r in range(parts - 1)] + [xs[d]]
                ys = mix_scaled(ys, [tangent[0]] * bits_of(parts))
                for r in range(parts):
                    index, minus = place(d, r, part)
                    out[index, b, p, r, at] = -ys[r] if minus else ys[r]
        out_copy(t).start()
        return carry
    lax.fori_loop(0, rq // 8, body, 0)
    for t in range(rq // 8):
        out_copy(t).wait()


def solution(mesh):
    nh, nl = mesh.shape["high"], mesh.shape["low"]
    n = nh * nl

    def on_device(wave, level, diag, turn):
        blocks, rows, lanes = level.shape
        rp = rows // (n // blocks)
        level = level.reshape(nh, 2, nl // 2, rp, lanes)
        parts = 2 if rp % 16 == 0 else 1
        hbm = pl.BlockSpec(memory_space=pltpu.HBM)
        vmem = pl.BlockSpec(memory_space=pltpu.VMEM)
        dma = pltpu.SemaphoreType.DMA
        home, tangent = pl.pallas_call(
            functools.partial(kernel, nh, nl, parts),
            out_shape=(pltpu.VMEM((n, parts, 2, rp // parts, lanes), F32), pltpu.VMEM((2, 8, lanes), F32)),
            in_specs=[hbm] * 4,
            out_specs=(vmem, vmem),
            scratch_shapes=[
                pltpu.VMEM(diag.shape, F32),
                pltpu.SMEM(turn.shape, F32),
                pltpu.VMEM(wave.shape, F32),
                pltpu.VMEM(level.shape, F32),
                pltpu.VMEM((nh, nl // 2, rp, lanes), F32),
                pltpu.VMEM((n, parts, 2 * rp // parts, lanes), F32),
                pltpu.VMEM((n, parts, 2 * rp // parts, lanes), F32),
                pltpu.VMEM((n, rp, lanes), F32),
                pltpu.VMEM((n, parts, 2, rp // parts, lanes), F32),
                pltpu.VMEM((2, 2 * lanes, 2 * lanes), BF16),
                pltpu.VMEM((2, 2 * rows, 2 * rows), BF16),
                dma((5,)), *[pltpu.SemaphoreType.REGULAR((bits_of(n),))] * 2, dma, dma, dma, dma, dma((parts,)), dma((parts,)),
                dma((parts,)), dma((parts,)),
            ],
            compiler_params=pltpu.CompilerParams(
                collective_id=0, has_side_effects=True, vmem_limit_bytes=20 * 2**20),
        )(*[pltpu.with_memory_space_constraint(x, pltpu.HBM) for x in (wave, level, diag, turn)])
        split_shape = (2, blocks, n // blocks, parts, rp // parts, lanes)
        out = pl.pallas_call(
            close,
            out_shape=jax.ShapeDtypeStruct(split_shape, F32),
            in_specs=[vmem, vmem],
            out_specs=hbm,
            scratch_shapes=[pltpu.VMEM(split_shape, F32), dma((rp // parts // 8,))],
            compiler_params=pltpu.CompilerParams(vmem_limit_bytes=8 * 2**20),
        )(home, tangent)
        return out.reshape(wave.shape)

    in_specs = (P(None, ("high", "low"), None, None), P(("high", "low"), None, None), P(), P())
    return jax.shard_map(
        on_device, mesh=mesh, in_specs=in_specs,
        out_specs=P(None, ("high", "low"), None, None), check_vma=False)
```
